8 devices in a mesh: dp: 1 (over z), ey: 2 (over y), ex: 4 (over x, core).
Axes of the slice: x: 2, y: 2, z: 1, core: 2. Of those that a mesh axis runs over, the one named last changes fastest.
Arguments:
- x: bfloat16 [1024, 2048], P(('dp', 'ey', 'ex'))
- ids: int32 [1024, 6], P(('dp', 'ey', 'ex'))
- gates: float32 [1024, 6], P(('dp', 'ey', 'ex'))
- w1: bfloat16 [64, 2048, 1408], P(('ey', 'ex'))
- w3: bfloat16 [64, 2048, 1408], P(('ey', 'ex'))
- w2: bfloat16 [64, 1408, 2048], P(('ey', 'ex'))
Outputs:
- output: bfloat16 [1024, 2048], P(('dp', 'ey', 'ex'))
All inputs are finite; a program needn't handle non-finite values.
Results may differ from the reference program's by a relative error of at most 0.00637368.
Values are sent between devices in bfloat16 or wider.
A program may use at most 1 GiB of HBM per device.

```python
import jax
import jax.numpy as jnp
from jax import lax

H = 2048
F = 1408
E = 64
TOP = 6
NG = 1
TG = 1
T = 128
P = 8

EL = E // P
N = P * T
GN = max(NG, 8)
GT = TG + (GN // 2 - TG) * (1 // NG)
EG = E // GN
CAP = min(T, 2 * T * TOP // P)


def setup_inputs(seed: int = 0, part: int = 0) -> dict:
    kw1, kw3, kw2 = jax.random.split(jax.random.key(seed), 3)
    kb1, kb2 = jax.random.split(jax.random.fold_in(jax.random.key(seed), 7), 2)
    kpart = jax.random.fold_in(jax.random.key(seed + 1), part)
    kx, _, _, ka = jax.random.split(kpart, 4)
    kg, ke = jax.random.split(jax.random.fold_in(kpart, 7), 2)
    x = jax.random.normal(kx, (N, H), jnp.float32)
    group_bias = jax.random.randint(kb1, (GN,), 0, 2 ** 21, jnp.int32)
    bias_draw = jax.random.randint(kb2, (E,), 0, 2 ** 10, jnp.int32)
    expert_bias = (3 * bias_draw * bias_draw) >> 1
    group_draw = jax.random.randint(kg, (N, GN), 0, 2 ** 20, jnp.int32)
    group_score = (group_draw + group_bias[None, :]) * GN + jnp.arange(GN, dtype=jnp.int32)[None, :]
    gtop = lax.top_k(group_score, GT)[1]
    gmask = jnp.any(gtop[:, :, None] == jnp.arange(GN)[None, None, :], axis=1)
    emask = jnp.repeat(gmask, EG, axis=1).astype(jnp.int32)
    expert_draw = jax.random.randint(ke, (N, E), 0, 2 ** 20, jnp.int32)
    expert_score = (expert_draw + expert_bias[None, :] + (4 << 20) * emask) * E + jnp.arange(E, dtype=jnp.int32)[None, :]
    ids = lax.top_k(expert_score, TOP)[1].astype(jnp.int32)
    a = jax.random.uniform(ka, (N, TOP), jnp.float32, 0.5, 1.5)
    gates = 2.5 * a / jnp.sum(a, axis=1, keepdims=True)
    w1 = jax.random.normal(kw1, (E, H, F), jnp.float32) * H ** -0.5
    w3 = jax.random.normal(kw3, (E, H, F), jnp.float32) * H ** -0.5
    w2 = jax.random.normal(kw2, (E, F, H), jnp.float32) * F ** -0.5
    return {"x": x.astype(jnp.bfloat16), "ids": ids, "gates": gates,
            "w1": w1.astype(jnp.bfloat16), "w3": w3.astype(jnp.bfloat16),
            "w2": w2.astype(jnp.bfloat16)}


def keep_mask(ids):
    dev = ids // EL
    hit = jnp.any(dev[:, :, None] == jnp.arange(P)[None, None, :], axis=1)
    hit3 = hit.reshape(P, T, P)
    rank = jnp.cumsum(hit3.astype(jnp.int32), axis=1) - 1
    kept = (hit3 & (rank < CAP)).reshape(N, P)
    return jnp.take_along_axis(kept, dev, axis=1)


def reference(x, ids, gates, w1, w3, w2):
    wk = gates * keep_mask(ids).astype(jnp.float32)

    def body(acc, e):
        c = jnp.sum(jnp.where(ids == e, wk, 0.0), axis=1)
        a1 = jnp.dot(x, w1[e], preferred_element_type=jnp.float32)
        a3 = jnp.dot(x, w3[e], preferred_element_type=jnp.float32)
        h = (jax.nn.silu(a1) * a3).astype(jnp.bfloat16)
        o = jnp.dot(h, w2[e], preferred_element_type=jnp.float32).astype(jnp.bfloat16)
        return acc + c[:, None] * o.astype(jnp.float32), None

    acc, _ = lax.scan(body, jnp.zeros((N, H), jnp.float32), jnp.arange(E))
    return (x.astype(jnp.float32) + acc).astype(jnp.bfloat16)
```

```python
import functools

import jax
import jax.numpy as jnp
from jax import lax
from jax.experimental import pallas as pl
from jax.experimental.pallas import tpu as pltpu
from jax.sharding import PartitionSpec as P

CAPF = 2
MESH = pl.DeviceIdType.MESH
ANY = pl.BlockSpec(memory_space=pl.ANY)
VM = pl.BlockSpec(memory_space=pltpu.VMEM)
SM = pl.BlockSpec(memory_space=pltpu.SMEM)
VLIM = 67043328


def place():
    dp, ey, ex = lax.axis_index("dp"), lax.axis_index("ey"), lax.axis_index("ex")
    ix, ic = ex // 2, ex % 2
    part = (dp, ey, ix * 2 + (1 - ic))
    xn = (dp, ey, (1 - ix) * 2 + ic)
    yn = (dp, 1 - ey, ex)
    return dp, ey, ix, ic, part, xn, yn


def gather_kernel(cap, x_ref, ids_ref, gates_ref, xall_ref, pos_ref, tok_ref, cum_ref,
                  meta, ssem, rsem, msend, mrecv):
    t, hd = x_ref.shape
    top = ids_ref.shape[1]
    hf = t // 2
    dp, ey, ix, ic, part, xn, yn = place()
    me = ey * 4 + ix * 2 + ic
    dxn = ey * 4 + (1 - ix) * 2 + ic
    dyn = (1 - ey) * 4 + ix * 2 + ic
    ddg = (1 - ey) * 4 + (1 - ix) * 2 + ic

    def dev(d):
        return (dp, d // 4, d % 4)

    pad = jnp.zeros((t, 8 - top), jnp.float32)
    both = jnp.concatenate([ids_ref[...].astype(jnp.float32), pad - 1.0,
                            gates_ref[...], pad, jnp.zeros((t, 112), jnp.float32)], axis=1)
    meta[me] = jnp.transpose(both)[:16]

    barrier = pltpu.get_barrier_semaphore()
    for j in range(1, 8):
        pl.semaphore_signal(barrier, inc=1, device_id=dev((me + j) % 8), device_id_type=MESH)
    pl.semaphore_wait(barrier, 7)

    mcopies = []
    for j in range(1, 8):
        c = pltpu.make_async_remote_copy(
            src_ref=meta.at[me], dst_ref=meta.at[me], send_sem=msend.at[j - 1],
            recv_sem=mrecv.at[j - 1], device_id=dev((me + j) % 8), device_id_type=MESH)
        c.start()
        mcopies.append(c)

    def rows(d, h):
        return pl.ds(pl.multiple_of(d * t + h * hf, hf), hf)

    def rc(k, src, d, h, to):
        return pltpu.make_async_remote_copy(
            src_ref=src, dst_ref=xall_ref.at[rows(d, h)], send_sem=ssem.at[k],
            recv_sem=rsem.at[k], device_id=to, device_id_type=MESH)

    def own(k, h, to):
        return rc(k, x_ref.at[pl.ds(h * hf, hf)], me, h, to)

    def fwd(k, d, h, to):
        return rc(k, xall_ref.at[rows(d, h)], d, h, to)

    cs = {0: own(0, 0, xn), 1: own(1, 1, xn), 2: own(2, 1, yn), 3: own(3, 0, yn),
          4: own(4, 0, part), 5: own(5, 1, part),
          6: fwd(6, dxn, 0, yn), 7: fwd(7, dyn, 1, xn),
          8: fwd(8, dxn, 0, part), 9: fwd(9, dxn, 1, part),
          10: fwd(10, dyn, 1, part), 11: fwd(11, dyn, 0, part),
          12: fwd(12, ddg, 0, part), 13: fwd(13, ddg, 1, part)}
    for k in (0, 2, 1, 3, 4, 5):
        cs[k].start()
    xall_ref[pl.ds(pl.multiple_of(me * t, t), t)] = x_ref[...]

    for c in mcopies:
        c.wait_recv()

    el = pos_ref.shape[0]
    ri = lax.broadcasted_iota(jnp.int32, (128, 128), 0)
    ci = lax.broadcasted_iota(jnp.int32, (128, 128), 1)
    upper = (ri < ci).astype(jnp.bfloat16)
    sub = lax.broadcasted_iota(jnp.int32, (el, t), 0)
    lane = lax.broadcasted_iota(jnp.int32, (el, 128), 1)
    base = jnp.zeros((el, 1), jnp.float32)
    cum = jnp.zeros((el, 128), jnp.float32)
    first = (me * el).astype(jnp.float32)
    for b in range(8):
        m = meta[b]
        idb, gb = m[:8], m[8:]
        mask = jnp.zeros((el, t), jnp.float32)
        coef = jnp.zeros((el, t), jnp.float32)
        for e in range(el):
            eq = idb == first + e
            mask = jnp.where(sub == e, jnp.max(jnp.where(eq, 1.0, 0.0), axis=0, keepdims=True), mask)
            coef = jnp.where(sub == e, jnp.sum(jnp.where(eq, gb, 0.0), axis=0, keepdims=True), coef)
        hit = jnp.broadcast_to(jnp.max(mask, axis=0, keepdims=True), (el, t))
        rank = jnp.dot(hit.astype(jnp.bfloat16), upper, preferred_element_type=jnp.float32)
        mask = jnp.where(rank < cap, mask, 0.0)
        within = jnp.dot(mask.astype(jnp.bfloat16), upper, preferred_element_type=jnp.float32)
        pos = jnp.where(mask > 0.0, within + base, -1.0)
        cum = jnp.where(lane == b, base, cum)
        base = base + jnp.sum(mask, axis=1, keepdims=True)
        pos_ref[:, b * t:(b + 1) * t] = pos
        tok_ref[b * t:(b + 1) * t, :] = jnp.transpose(
            jnp.concatenate([pos, coef, jnp.zeros((128 - 2 * el, t), jnp.float32)], axis=0))
    cum_ref[...] = jnp.where(lane == 8, base, cum).astype(jnp.int32)

    cs[0].wait_recv()
    cs[6].start()
    cs[8].start()
    cs[2].wait_recv()
    cs[7].start()
    cs[10].start()
    cs[1].wait_recv()
    cs[9].start()
    cs[3].wait_recv()
    cs[11].start()
    cs[6].wait_recv()
    cs[12].start()
    cs[7].wait_recv()
    cs[13].start()
    for k in (4, 5, 8, 9, 10, 11, 12, 13):
        cs[k].wait_recv()
    for k in range(14):
        cs[k].wait_send()
    for c in mcopies:
        c.wait_send()


def expert_kernel(cum_ref, pos_ref, tok_ref, x_ref, w1_ref, w3_ref, w2_ref, acc_ref,
                  w13b, w2b, xg, ob, order, sems):
    el, hd, f = w1_ref.shape
    n = x_ref.shape[0]
    tb = 256
    nb = n // tb
    per = tb // 128

    def listing(e, k):
        @pl.when(cum_ref[e, 8] > 0)
        def _():
            order[k] = e
        return jnp.where(cum_ref[e, 8] > 0, k + 1, k)

    nact = lax.fori_loop(0, el, listing, 0)

    def copies(k):
        e, s = order[k], k % 2
        return (pltpu.make_async_copy(w1_ref.at[e], w13b.at[s, :, pl.ds(0, f)], sems.at[s, 0]),
                pltpu.make_async_copy(w3_ref.at[e], w13b.at[s, :, pl.ds(f, f)], sems.at[s, 1]),
                pltpu.make_async_copy(w2_ref.at[e], w2b.at[s], sems.at[s, 2]))

    def start(k):
        @pl.when(k < nact)
        def _():
            for c in copies(k):
                c.start()

    start(0)
    start(1)
    acc_ref[...] = jnp.zeros_like(acc_ref)

    def tile(e, s, r0, tm):
        def overlap(b):
            return (cum_ref[e, b * per] < r0 + tm) & (cum_ref[e, (b + 1) * per] > r0)

        r0f = r0.astype(jnp.float32)
        xg[:tm] = jnp.zeros((tm, hd), xg.dtype)

        def pick(b, c):
            @pl.when(overlap(b))
            def _():
                toks = pl.ds(pl.multiple_of(b * tb, tb), tb)
                p = pos_ref[pl.ds(e, 1), toks]
                rows = lax.broadcasted_iota(jnp.int32, (tm, tb), 0).astype(jnp.float32) + r0f
                sel = jnp.where(rows == p, 1.0, 0.0).astype(jnp.bfloat16)
                xg[:tm] += jnp.dot(sel, x_ref[toks, :], preferred_element_type=jnp.float32).astype(xg.dtype)
            return c

        lax.fori_loop(0, nb, pick, 0)
        a = jnp.dot(xg[:tm], w13b[s], preferred_element_type=jnp.float32)
        a1, a3 = a[:, :f], a[:, f:]
        h = (jax.nn.silu(a1) * a3).astype(jnp.bfloat16)
        ob[:tm] = jnp.dot(h, w2b[s], preferred_element_type=jnp.float32).astype(jnp.bfloat16)

        def put(b, c):
            @pl.when(overlap(b))
            def _():
                toks = pl.ds(pl.multiple_of(b * tb, tb), tb)
                tk = tok_ref[toks, :]
                lane = lax.broadcasted_iota(jnp.int32, tk.shape, 1)
                p = jnp.sum(jnp.where(lane == e, tk, 0.0), axis=1, keepdims=True)
                g = jnp.sum(jnp.where(lane == el + e, tk, 0.0), axis=1, keepdims=True)
                rows = lax.broadcasted_iota(jnp.int32, (tb, tm), 1).astype(jnp.float32) + r0f
                sel = jnp.where(rows == p, 1.0, 0.0).astype(jnp.bfloat16)
                acc_ref[toks, :] += g * jnp.dot(sel, ob[:tm], preferred_element_type=jnp.float32)
            return c

        lax.fori_loop(0, nb, put, 0)

    def expert(k, c):
        e, s = order[k], k % 2
        for cp in copies(k):
            cp.wait()
        cnt = cum_ref[e, 8]
        rem = cnt % 256
        big = cnt // 256 + jnp.where(rem > 128, 1, 0)

        def step(i, c):
            tile(e, s, i * 256, 256)
            return c

        lax.fori_loop(0, big, step, 0)

        @pl.when((rem > 0) & (rem <= 128))
        def _():
            tile(e, s, big * 256, 128)

        start(k + 2)
        return c

    lax.fori_loop(0, nact, expert, 0)


def scatter_kernel(nc, part_ref, x_ref, y_ref, own, prt, rx, ry, r2, lsem, s0, q0, s1, q1, s2, q2):
    dp, ey, ix, ic, part, xn, yn = place()
    hd = x_ref.shape[1]
    half = hd // 2
    w = half // nc
    barrier = pltpu.get_barrier_semaphore()
    for d in (part, xn, yn):
        pl.semaphore_signal(barrier, inc=1, device_id=d, device_id_type=MESH)

    chunks = [(s, i) for i in range(nc) for s in range(2)]

    def cols(s, i):
        return pl.ds(s * half + i * w, w)

    loads, ph0, ph1, ph2 = {}, {}, {}, {}
    for s, i in chunks:
        k = i * 2 + s
        c = cols(s, i)
        loads[s, i] = pltpu.make_async_copy(part_ref.at[:, :, ic, :, c], own.at[:, :, :, c], lsem.at[k])
        ph0[s, i] = pltpu.make_async_remote_copy(
            src_ref=part_ref.at[:, :, 1 - ic, :, c], dst_ref=prt.at[:, :, :, c], send_sem=s0.at[k],
            recv_sem=q0.at[k], device_id=part, device_id_type=MESH)
        if s == 0:
            ph1[s, i] = pltpu.make_async_remote_copy(
                src_ref=own.at[:, 1 - ix, :, c], dst_ref=rx.at[:, :, pl.ds(i * w, w)], send_sem=s1.at[k],
                recv_sem=q1.at[k], device_id=xn, device_id_type=MESH)
            ph2[s, i] = pltpu.make_async_remote_copy(
                src_ref=own.at[1 - ey, ix, :, c], dst_ref=r2.at[:, c], send_sem=s2.at[k],
                recv_sem=q2.at[k], device_id=yn, device_id_type=MESH)
        else:
            ph1[s, i] = pltpu.make_async_remote_copy(
                src_ref=own.at[1 - ey, :, :, c], dst_ref=ry.at[:, :, pl.ds(i * w, w)], send_sem=s1.at[k],
                recv_sem=q1.at[k], device_id=yn, device_id_type=MESH)
            ph2[s, i] = pltpu.make_async_remote_copy(
                src_ref=own.at[ey, 1 - ix, :, c], dst_ref=r2.at[:, c], send_sem=s2.at[k],
                recv_sem=q2.at[k], device_id=xn, device_id_type=MESH)
    for k in chunks:
        loads[k].start()
    pl.semaphore_wait(barrier, 3)
    for k in chunks:
        ph0[k].start()
    for s, i in chunks:
        c = cols(s, i)
        loads[s, i].wait()
        ph0[s, i].wait_recv()
        if s == 0:
            own[:, 1 - ix, :, c] += prt[:, 1 - ix, :, c]
        else:
            own[1 - ey, :, :, c] += prt[1 - ey, :, :, c]
        ph1[s, i].start()
        if s == 0:
            own[:, ix, :, c] += prt[:, ix, :, c]
        else:
            own[ey, :, :, c] += prt[ey, :, :, c]
    for s, i in chunks:
        c = cols(s, i)
        ph1[s, i].wait_recv()
        if s == 0:
            own[1 - ey, ix, :, c] += rx[1 - ey, :, i * w:(i + 1) * w]
        else:
            own[ey, 1 - ix, :, c] += ry[1 - ix, :, i * w:(i + 1) * w]
        ph2[s, i].start()
        if s == 0:
            own[ey, ix, :, c] += rx[ey, :, i * w:(i + 1) * w]
        else:
            own[ey, ix, :, c] += ry[ix, :, i * w:(i + 1) * w]
    for s, i in chunks:
        c = cols(s, i)
        ph2[s, i].wait_recv()
        y_ref[:, c] = (x_ref[:, c].astype(jnp.float32) + (own[ey, ix, :, c] + r2[:, c])).astype(y_ref.dtype)
    for k in chunks:
        ph0[k].wait_send()
        ph1[k].wait_send()
        ph2[k].wait_send()


def solution(mesh):
    nx = mesh.shape["ex"]
    nd = mesh.shape["ey"] * nx
    tok = P(("dp", "ey", "ex"), None)
    wsp = P(("ey", "ex"), None, None)
    f32 = jnp.float32
    dma = pltpu.SemaphoreType.DMA

    def local(x, ids, gates, w1, w3, w2):
        t, hd = x.shape
        top = ids.shape[1]
        el, _, f = w1.shape
        n = nd * t
        cap = min(t, CAPF * t * top // nd)
        xall, pos, tokt, cum = pl.pallas_call(
            functools.partial(gather_kernel, cap),
            out_shape=(jax.ShapeDtypeStruct((n, hd), x.dtype), jax.ShapeDtypeStruct((el, n), f32),
                       jax.ShapeDtypeStruct((n, 128), f32), jax.ShapeDtypeStruct((el, 128), jnp.int32)),
            in_specs=[VM] * 3, out_specs=(VM,) * 4,
            scratch_shapes=[pltpu.VMEM((nd, 16, t), f32), dma((14,)), dma((14,)), dma((7,)), dma((7,))],
            compiler_params=pltpu.CompilerParams(collective_id=0, has_side_effects=True),
            name="gather")(x, ids, gates)
        acc = pl.pallas_call(
            expert_kernel,
            out_shape=jax.ShapeDtypeStruct((n, hd), f32),
            in_specs=[SM, VM, VM, VM, ANY, ANY, ANY], out_specs=VM,
            scratch_shapes=[pltpu.VMEM((2, hd, 2 * f), w1.dtype), pltpu.VMEM((2, f, hd), w2.dtype),
                            pltpu.VMEM((256, hd), x.dtype), pltpu.VMEM((256, hd), x.dtype),
                            pltpu.SMEM((el + 2,), jnp.int32), dma((2, 3))],
            compiler_params=pltpu.CompilerParams(vmem_limit_bytes=VLIM),
            name="experts")(cum, pos, tokt, xall, w1, w3, w2)
        nc = 4
        half = hd // 2
        y = pl.pallas_call(
            functools.partial(scatter_kernel, nc),
            out_shape=jax.ShapeDtypeStruct((t, hd), x.dtype),
            in_specs=[ANY, VM], out_specs=VM,
            scratch_shapes=[pltpu.VMEM((2, 2, t, hd), f32), pltpu.VMEM((2, 2, t, hd), f32),
                            pltpu.VMEM((2, t, half), f32), pltpu.VMEM((2, t, half), f32),
                            pltpu.VMEM((t, hd), f32)] + [dma((2 * nc,))] * 7,
            compiler_params=pltpu.CompilerParams(collective_id=1, has_side_effects=True),
            name="scatter")(acc.reshape(2, 2, 2, t, hd), x)
        return y

    return jax.shard_map(local, mesh=mesh, in_specs=(tok, tok, tok, wsp, wsp, wsp),
                         out_specs=tok, check_vma=False)
```

```python
import functools

import jax
import jax.numpy as jnp
from jax import lax
from jax.experimental import pallas as pl
from jax.experimental.pallas import tpu as pltpu
from jax.sharding import PartitionSpec as P

CAPF = 2
MESH = pl.DeviceIdType.MESH
ANY = pl.BlockSpec(memory_space=pl.ANY)
VM = pl.BlockSpec(memory_space=pltpu.VMEM)
SM = pl.BlockSpec(memory_space=pltpu.SMEM)
VLIM = 67043328


def place():
    dp, ey, ex = lax.axis_index("dp"), lax.axis_index("ey"), lax.axis_index("ex")
    ix, ic = ex // 2, ex % 2
    part = (dp, ey, ix * 2 + (1 - ic))
    xn = (dp, ey, (1 - ix) * 2 + ic)
    yn = (dp, 1 - ey, ex)
    return dp, ey, ix, ic, part, xn, yn


def gather_kernel(cap, x_ref, ids_ref, gates_ref, out_ref, pos_ref, tok_ref, cum_ref,
                  xall_ref, meta, ssem, rsem, osem, msend, mrecv):
    t, hd = x_ref.shape
    top = ids_ref.shape[0]
    hf = t // 2
    dp, ey, ix, ic, part, xn, yn = place()
    me = ey * 4 + ix * 2 + ic
    dxn = ey * 4 + (1 - ix) * 2 + ic
    dyn = (1 - ey) * 4 + ix * 2 + ic
    ddg = (1 - ey) * 4 + (1 - ix) * 2 + ic

    def dev(d):
        return (dp, d // 4, d % 4)

    meta[me, :top] = ids_ref[...].astype(jnp.float32)
    meta[me, top:8] = jnp.full((8 - top, t), -1.0, jnp.float32)
    meta[me, 8:8 + top] = gates_ref[...]
    meta[me, 8 + top:] = jnp.zeros((8 - top, t), jnp.float32)

    barrier = pltpu.get_barrier_semaphore()
    for j in range(1, 8):
        pl.semaphore_signal(barrier, inc=1, device_id=dev((me + j) % 8), device_id_type=MESH)
    pl.semaphore_wait(barrier, 7)

    mcopies = []
    for j in range(1, 8):
        c = pltpu.make_async_remote_copy(
            src_ref=meta.at[me], dst_ref=meta.at[me], send_sem=msend.at[j - 1],
            recv_sem=mrecv.at[j - 1], device_id=dev((me + j) % 8), device_id_type=MESH)
        c.start()
        mcopies.append(c)

    def rows(d, h):
        return pl.ds(pl.multiple_of(d * t + h * hf, hf), hf)

    def rc(k, src, d, h, to):
        return pltpu.make_async_remote_copy(
            src_ref=src, dst_ref=xall_ref.at[rows(d, h)], send_sem=ssem.at[k],
            recv_sem=rsem.at[k], device_id=to, device_id_type=MESH)

    def own(k, h, to):
        return rc(k, x_ref.at[pl.ds(h * hf, hf)], me, h, to)

    def fwd(k, d, h, to):
        return rc(k, xall_ref.at[rows(d, h)], d, h, to)

    cs = {0: own(0, 0, xn), 1: own(1, 1, xn), 2: own(2, 1, yn), 3: own(3, 0, yn),
          4: own(4, 0, part), 5: own(5, 1, part),
          6: fwd(6, dxn, 0, yn), 7: fwd(7, dyn, 1, xn),
          8: fwd(8, dxn, 0, part), 9: fwd(9, dxn, 1, part),
          10: fwd(10, dyn, 1, part), 11: fwd(11, dyn, 0, part),
          12: fwd(12, ddg, 0, part), 13: fwd(13, ddg, 1, part)}
    for k in (0, 2, 1, 3, 4, 5):
        cs[k].start()

    outs = []

    def out(d, h):
        src = x_ref.at[pl.ds(h * hf, hf)] if d is None else xall_ref.at[rows(d, h)]
        o = pltpu.make_async_copy(src, out_ref.at[rows(me if d is None else d, h)], osem.at[len(outs)])
        o.start()
        outs.append(o)

    out(None, 0)
    out(None, 1)

    for c in mcopies:
        c.wait_recv()

    el = pos_ref.shape[0]
    ri = lax.broadcasted_iota(jnp.int32, (128, 128), 0)
    ci = lax.broadcasted_iota(jnp.int32, (128, 128), 1)
    upper = (ri < ci).astype(jnp.bfloat16)
    sub = lax.broadcasted_iota(jnp.int32, (el, t), 0)
    lane = lax.broadcasted_iota(jnp.int32, (el, 128), 1)
    base = jnp.zeros((el, 1), jnp.float32)
    cum = jnp.zeros((el, 128), jnp.float32)
    first = (me * el).astype(jnp.float32)
    for b in range(8):
        m = meta[b]
        idb, gb = m[:8], m[8:]
        mask = jnp.zeros((el, t), jnp.float32)
        coef = jnp.zeros((el, t), jnp.float32)
        for e in range(el):
            eq = idb == first + e
            mask = jnp.where(sub == e, jnp.max(jnp.where(eq, 1.0, 0.0), axis=0, keepdims=True), mask)
            coef = jnp.where(sub == e, jnp.sum(jnp.where(eq, gb, 0.0), axis=0, keepdims=True), coef)
        hit = jnp.broadcast_to(jnp.max(mask, axis=0, keepdims=True), (el, t))
        rank = jnp.dot(hit.astype(jnp.bfloat16), upper, preferred_element_type=jnp.float32)
        mask = jnp.where(rank < cap, mask, 0.0)
        within = jnp.dot(mask.astype(jnp.bfloat16), upper, preferred_element_type=jnp.float32)
        pos = jnp.where(mask > 0.0, within + base, -1.0)
        cum = jnp.where(lane == b, base, cum)
        base = base + jnp.sum(mask, axis=1, keepdims=True)
        pos_ref[:, b * t:(b + 1) * t] = pos
        tok_ref[b * t:(b + 1) * t, :] = jnp.transpose(
            jnp.concatenate([pos, coef, jnp.zeros((128 - 2 * el, t), jnp.float32)], axis=0))
    cum_ref[...] = jnp.where(lane == 8, base, cum).astype(jnp.int32)

    pxn, pyn, pdg, pme = [d + 1 - 2 * ic for d in (dxn, dyn, ddg, me)]
    for k, d, h, then in ((0, dxn, 0, (6, 8)), (2, dyn, 1, (7, 10)), (4, pme, 0, ()), (5, pme, 1, ()),
                          (1, dxn, 1, (9,)), (3, dyn, 0, (11,)), (8, pxn, 0, ()), (10, pyn, 1, ()),
                          (9, pxn, 1, ()), (11, pyn, 0, ()), (6, ddg, 0, (12,)), (7, ddg, 1, (13,)),
                          (12, pdg, 0, ()), (13, pdg, 1, ())):
        cs[k].wait_recv()
        for f in then:
            cs[f].start()
        out(d, h)
    for k in range(14):
        cs[k].wait_send()
    for c in mcopies:
        c.wait_send()
    for o in outs:
        o.wait()


def expert_kernel(cum_ref, pos_ref, tok_ref, x_hbm, w1_ref, w3_ref, w2_ref, acc_ref,
                  w13b, w2b, x_ref, sel, gcol, xg, hb, ob, order, sems, xsem):
    el, hd, f = w1_ref.shape
    n = x_hbm.shape[0]
    tb = 256
    dense_from = 768

    def listing(e, k):
        @pl.when(cum_ref[e, 8] > 0)
        def _():
            order[k] = e
        return jnp.where(cum_ref[e, 8] > 0, k + 1, k)

    nact = lax.fori_loop(0, el, listing, 0)

    def up(k):
        e, s = order[k], k % 2
        return (pltpu.make_async_copy(w1_ref.at[e], w13b.at[s, :, pl.ds(0, f)], sems.at[s, 0]),
                pltpu.make_async_copy(w3_ref.at[e], w13b.at[s, :, pl.ds(f, f)], sems.at[s, 1]))

    def down(k):
        e, s = order[k], k % 2
        return (pltpu.make_async_copy(w2_ref.at[e], w2b.at[s], sems.at[s, 2]),)

    def start(copies, k):
        @pl.when(k < nact)
        def _():
            for c in copies(k):
                c.start()

    start(up, 0)
    xcopy = pltpu.make_async_copy(x_hbm, x_ref, xsem)
    xcopy.start()
    start(down, 0)
    start(up, 1)
    start(down, 1)
    acc_ref[...] = jnp.zeros_like(acc_ref)
    xcopy.wait()

    def tile(k, e, s, r0, tm, cnt, dense):
        first, last = r0 == 0, r0 + tm >= jnp.where(dense, n, cnt)
        r0f = r0.astype(jnp.float32)
        lo = jnp.int32(0)
        hi = jnp.int32(0)
        for b in range(8):
            lo += jnp.where(cum_ref[e, b + 1] <= r0, 1, 0)
            hi += jnp.where(cum_ref[e, b] < r0 + tm, 1, 0)
        narrow = hi - lo <= 4
        w0 = jnp.where(narrow, jnp.minimum(lo, 4), 0)

        def pick(win):
            toks = pl.ds(pl.multiple_of(w0 * 128, 128), win)
            p = pos_ref[pl.ds(e, 1), toks]
            rows = lax.broadcasted_iota(jnp.int32, (tm, win), 0).astype(jnp.float32) + r0f
            sel[:tm, :win] = jnp.where(rows == p, 1.0, 0.0).astype(jnp.bfloat16)
            xg[:tm] = jnp.dot(sel[:tm, :win], x_ref[toks, :], preferred_element_type=jnp.float32).astype(xg.dtype)

        if tm == 256:
            @pl.when(dense)
            def _():
                xg[:tm] = x_ref[pl.ds(pl.multiple_of(r0, tm), tm), :]

        @pl.when(jnp.logical_not(dense) & narrow)
        def _():
            pick(512)

        @pl.when(jnp.logical_not(dense) & jnp.logical_not(narrow))
        def _():
            pick(1024)

        @pl.when(first)
        def _():
            for c in up(k):
                c.wait()

        a = jnp.dot(xg[:tm], w13b[s], preferred_element_type=jnp.float32)
        a1, a3 = a[:, :f], a[:, f:]
        hb[:tm] = (jax.nn.silu(a1) * a3).astype(jnp.bfloat16)

        @pl.when(last)
        def _():
            start(up, k + 2)

        @pl.when(first)
        def _():
            for c in down(k):
                c.wait()

        ob[:tm] = jnp.dot(hb[:tm], w2b[s], preferred_element_type=jnp.float32).astype(jnp.bfloat16)

        @pl.when(last)
        def _():
            start(down, k + 2)

        if tm == 256:
            @pl.when(dense)
            def _():
                toks = pl.ds(pl.multiple_of(r0, tm), tm)
                g = gcol[toks, :1]
                acc_ref[toks, :] += jnp.where(g > 0.0, g * ob[:tm].astype(jnp.float32), 0.0)

        def put(i, c):
            b = w0 + 2 * i

            @pl.when((cum_ref[e, b] < r0 + tm) & (cum_ref[e, b + 2] > r0))
            def _():
                toks = pl.ds(pl.multiple_of(b * 128, 128), tb)
                sl = sel[:tm, pl.ds(pl.multiple_of(i * tb, tb), tb)]
                r = lax.dot_general(sl, ob[:tm], (((0,), (0,)), ((), ())), preferred_element_type=jnp.float32)
                acc_ref[toks, :] += gcol[toks, :1] * r
            return c

        lax.fori_loop(0, jnp.where(dense, 0, jnp.where(narrow, 2, 4)), put, 0)

    def expert(k, c):
        e, s = order[k], k % 2

        def column(b, c):
            toks = pl.ds(pl.multiple_of(b * 128, 128), 128)
            tk = tok_ref[toks, :]
            lane = lax.broadcasted_iota(jnp.int32, tk.shape, 1)
            g = jnp.sum(jnp.where(lane == el + e, tk, 0.0), axis=1, keepdims=True)
            gcol[toks, :] = jnp.broadcast_to(g, tk.shape)
            return c

        lax.fori_loop(0, n // 128, column, 0)
        cnt = cum_ref[e, 8]
        dense = cnt > dense_from
        rem = jnp.where(dense, 0, cnt % 256)
        big = jnp.where(dense, n // 256, cnt // 256 + jnp.where(rem > 128, 1, 0))

        def step(i, c):
            tile(k, e, s, i * 256, 256, cnt, dense)
            return c

        lax.fori_loop(0, big, step, 0)

        @pl.when((rem > 0) & (rem <= 128))
        def _():
            tile(k, e, s, big * 256, 128, cnt, jnp.bool_(False))

        return c

    lax.fori_loop(0, nact, expert, 0)


def scatter_kernel(nc, part_ref, x_ref, y_ref, own, prt, rx, ry, r2, lsem, s0, q0, s1, q1, s2, q2):
    dp, ey, ix, ic, part, xn, yn = place()
    hd = x_ref.shape[1]
    half = hd // 2
    w = half // nc
    barrier = pltpu.get_barrier_semaphore()
    for d in (part, xn, yn):
        pl.semaphore_signal(barrier, inc=1, device_id=d, device_id_type=MESH)

    chunks = [(s, i) for i in range(nc) for s in range(2)]

    def cols(s, i):
        return pl.ds(s * half + i * w, w)

    loads, ph0, ph1, ph2 = {}, {}, {}, {}
    for s, i in chunks:
        k = i * 2 + s
        c = cols(s, i)
        loads[s, i] = pltpu.make_async_copy(part_ref.at[:, :, ic, :, c], own.at[:, :, :, c], lsem.at[k])
        ph0[s, i] = pltpu.make_async_remote_copy(
            src_ref=part_ref.at[:, :, 1 - ic, :, c], dst_ref=prt.at[:, :, :, c], send_sem=s0.at[k],
            recv_sem=q0.at[k], device_id=part, device_id_type=MESH)
        if s == 0:
            ph1[s, i] = pltpu.make_async_remote_copy(
                src_ref=own.at[:, 1 - ix, :, c], dst_ref=rx.at[:, :, pl.ds(i * w, w)], send_sem=s1.at[k],
                recv_sem=q1.at[k], device_id=xn, device_id_type=MESH)
            ph2[s, i] = pltpu.make_async_remote_copy(
                src_ref=own.at[1 - ey, ix, :, c], dst_ref=r2.at[:, c], send_sem=s2.at[k],
                recv_sem=q2.at[k], device_id=yn, device_id_type=MESH)
        else:
            ph1[s, i] = pltpu.make_async_remote_copy(
                src_ref=own.at[1 - ey, :, :, c], dst_ref=ry.at[:, :, pl.ds(i * w, w)], send_sem=s1.at[k],
                recv_sem=q1.at[k], device_id=yn, device_id_type=MESH)
            ph2[s, i] = pltpu.make_async_remote_copy(
                src_ref=own.at[ey, 1 - ix, :, c], dst_ref=r2.at[:, c], send_sem=s2.at[k],
                recv_sem=q2.at[k], device_id=xn, device_id_type=MESH)
    for k in chunks:
        loads[k].start()
    pl.semaphore_wait(barrier, 3)
    for k in chunks:
        ph0[k].start()
    for s, i in chunks:
        c = cols(s, i)
        loads[s, i].wait()
        ph0[s, i].wait_recv()
        if s == 0:
            own[:, 1 - ix, :, c] += prt[:, 1 - ix, :, c]
        else:
            own[1 - ey, :, :, c] += prt[1 - ey, :, :, c]
        ph1[s, i].start()
        if s == 0:
            own[:, ix, :, c] += prt[:, ix, :, c]
        else:
            own[ey, :, :, c] += prt[ey, :, :, c]
    for s, i in chunks:
        c = cols(s, i)
        ph1[s, i].wait_recv()
        if s == 0:
            own[1 - ey, ix, :, c] += rx[1 - ey, :, i * w:(i + 1) * w]
        else:
            own[ey, 1 - ix, :, c] += ry[1 - ix, :, i * w:(i + 1) * w]
        ph2[s, i].start()
        if s == 0:
            own[ey, ix, :, c] += rx[ey, :, i * w:(i + 1) * w]
        else:
            own[ey, ix, :, c] += ry[ix, :, i * w:(i + 1) * w]
    for s, i in chunks:
        c = cols(s, i)
        ph2[s, i].wait_recv()
        y_ref[:, c] = (x_ref[:, c].astype(jnp.float32) + (own[ey, ix, :, c] + r2[:, c])).astype(y_ref.dtype)
    for k in chunks:
        ph0[k].wait_send()
        ph1[k].wait_send()
        ph2[k].wait_send()


def solution(mesh):
    nx = mesh.shape["ex"]
    nd = mesh.shape["ey"] * nx
    tok = P(("dp", "ey", "ex"), None)
    wsp = P(("ey", "ex"), None, None)
    f32 = jnp.float32
    dma = pltpu.SemaphoreType.DMA

    def local(x, ids, gates, w1, w3, w2):
        t, hd = x.shape
        top = ids.shape[1]
        el, _, f = w1.shape
        n = nd * t
        cap = min(t, CAPF * t * top // nd)
        xall, pos, tokt, cum = pl.pallas_call(
            functools.partial(gather_kernel, cap),
            out_shape=(jax.ShapeDtypeStruct((n, hd), x.dtype), jax.ShapeDtypeStruct((el, n), f32),
                       jax.ShapeDtypeStruct((n, 128), f32), jax.ShapeDtypeStruct((el, 128), jnp.int32)),
            in_specs=[VM] * 3, out_specs=(ANY, VM, VM, VM),
            scratch_shapes=[pltpu.VMEM((n, hd), x.dtype), pltpu.VMEM((nd, 16, t), f32),
                            dma((14,)), dma((14,)), dma((16,)), dma((7,)), dma((7,))],
            compiler_params=pltpu.CompilerParams(collective_id=0, has_side_effects=True),
            name="gather")(x, ids.T, gates.T)
        acc = pl.pallas_call(
            expert_kernel,
            out_shape=jax.ShapeDtypeStruct((n, hd), f32),
            in_specs=[SM, VM, VM, ANY, ANY, ANY, ANY], out_specs=VM,
            scratch_shapes=[pltpu.VMEM((2, hd, 2 * f), w1.dtype), pltpu.VMEM((2, f, hd), w2.dtype),
                            pltpu.VMEM((n, hd), x.dtype), pltpu.VMEM((256, n), x.dtype),
                            pltpu.VMEM((n, 128), f32), pltpu.VMEM((256, hd), x.dtype),
                            pltpu.VMEM((256, f), x.dtype), pltpu.VMEM((256, hd), x.dtype),
                            pltpu.SMEM((el + 2,), jnp.int32), dma((2, 3)), dma],
            compiler_params=pltpu.CompilerParams(vmem_limit_bytes=VLIM),
            name="experts")(cum, pos, tokt, xall, w1, w3, w2)
        nc = 4
        half = hd // 2
        y = pl.pallas_call(
            functools.partial(scatter_kernel, nc),
            out_shape=jax.ShapeDtypeStruct((t, hd), x.dtype),
            in_specs=[ANY, VM], out_specs=VM,
            scratch_shapes=[pltpu.VMEM((2, 2, t, hd), f32), pltpu.VMEM((2, 2, t, hd), f32),
                            pltpu.VMEM((2, t, half), f32), pltpu.VMEM((2, t, half), f32),
                            pltpu.VMEM((t, hd), f32)] + [dma((2 * nc,))] * 7,
            compiler_params=pltpu.CompilerParams(collective_id=1, has_side_effects=True),
            name="scatter")(acc.reshape(2, 2, 2, t, hd), x)
        return y

    return jax.shard_map(local, mesh=mesh, in_specs=(tok, tok, tok, wsp, wsp, wsp),
                         out_specs=tok, check_vma=False)
```

```python
import functools

import jax
import jax.numpy as jnp
from jax import lax
from jax.experimental import pallas as pl
from jax.experimental.pallas import tpu as pltpu
from jax.sharding import PartitionSpec as P

CAPF = 2
MESH = pl.DeviceIdType.MESH
ANY = pl.BlockSpec(memory_space=pl.ANY)
VM = pl.BlockSpec(memory_space=pltpu.VMEM)
SM = pl.BlockSpec(memory_space=pltpu.SMEM)
VLIM = 67043328


def place():
    dp, ey, ex = lax.axis_index("dp"), lax.axis_index("ey"), lax.axis_index("ex")
    ix, ic = ex // 2, ex % 2
    part = (dp, ey, ix * 2 + (1 - ic))
    xn = (dp, ey, (1 - ix) * 2 + ic)
    yn = (dp, 1 - ey, ex)
    return dp, ey, ix, ic, part, xn, yn


def gather_kernel(cap, x_ref, ids_ref, gates_ref, out_ref, pos_ref, gate_ref, cum_ref,
                  xall_ref, meta, slab, ssem, rsem, osem, gsem, msend, mrecv):
    t, hd = x_ref.shape
    top = ids_ref.shape[0]
    hf = t // 2
    dp, ey, ix, ic, part, xn, yn = place()
    me = ey * 4 + ix * 2 + ic
    dxn = ey * 4 + (1 - ix) * 2 + ic
    dyn = (1 - ey) * 4 + ix * 2 + ic
    ddg = (1 - ey) * 4 + (1 - ix) * 2 + ic

    def dev(d):
        return (dp, d // 4, d % 4)

    meta[me, :top] = ids_ref[...].astype(jnp.float32)
    meta[me, top:8] = jnp.full((8 - top, t), -1.0, jnp.float32)
    meta[me, 8:8 + top] = gates_ref[...]
    meta[me, 8 + top:] = jnp.zeros((8 - top, t), jnp.float32)

    barrier = pltpu.get_barrier_semaphore()
    for j in range(1, 8):
        pl.semaphore_signal(barrier, inc=1, device_id=dev((me + j) % 8), device_id_type=MESH)
    pl.semaphore_wait(barrier, 7)

    mcopies = []
    for j in range(1, 8):
        c = pltpu.make_async_remote_copy(
            src_ref=meta.at[me], dst_ref=meta.at[me], send_sem=msend.at[j - 1],
            recv_sem=mrecv.at[j - 1], device_id=dev((me + j) % 8), device_id_type=MESH)
        c.start()
        mcopies.append(c)

    def rows(d, h):
        return pl.ds(pl.multiple_of(d * t + h * hf, hf), hf)

    def rc(k, src, d, h, to):
        return pltpu.make_async_remote_copy(
            src_ref=src, dst_ref=xall_ref.at[rows(d, h)], send_sem=ssem.at[k],
            recv_sem=rsem.at[k], device_id=to, device_id_type=MESH)

    def own(k, h, to):
        return rc(k, x_ref.at[pl.ds(h * hf, hf)], me, h, to)

    def fwd(k, d, h, to):
        return rc(k, xall_ref.at[rows(d, h)], d, h, to)

    cs = {0: own(0, 0, xn), 1: own(1, 1, xn), 2: own(2, 1, yn), 3: own(3, 0, yn),
          4: own(4, 0, part), 5: own(5, 1, part),
          6: fwd(6, dxn, 0, yn), 7: fwd(7, dyn, 1, xn),
          8: fwd(8, dxn, 0, part), 9: fwd(9, dxn, 1, part),
          10: fwd(10, dyn, 1, part), 11: fwd(11, dyn, 0, part),
          12: fwd(12, ddg, 0, part), 13: fwd(13, ddg, 1, part)}
    for k in (0, 2, 1, 3, 4, 5):
        cs[k].start()

    outs = []

    def out(d, h):
        src = x_ref.at[pl.ds(h * hf, hf)] if d is None else xall_ref.at[rows(d, h)]
        o = pltpu.make_async_copy(src, out_ref.at[rows(me if d is None else d, h)], osem.at[len(outs)])
        o.start()
        outs.append(o)

    out(None, 0)
    out(None, 1)

    for c in mcopies:
        c.wait_recv()

    el = pos_ref.shape[0]
    ri = lax.broadcasted_iota(jnp.int32, (128, 128), 0)
    ci = lax.broadcasted_iota(jnp.int32, (128, 128), 1)
    upper = (ri < ci).astype(jnp.bfloat16)
    sub = lax.broadcasted_iota(jnp.int32, (el, t), 0)
    lane = lax.broadcasted_iota(jnp.int32, (el, 128), 1)
    base = jnp.zeros((el, 1), jnp.float32)
    cum = jnp.zeros((el, 128), jnp.float32)
    first = (me * el).astype(jnp.float32)
    for b in range(8):
        m = meta[b]
        idb, gb = m[:8], m[8:]
        mask = jnp.zeros((el, t), jnp.float32)
        coef = jnp.zeros((el, t), jnp.float32)
        for e in range(el):
            eq = idb == first + e
            mask = jnp.where(sub == e, jnp.max(jnp.where(eq, 1.0, 0.0), axis=0, keepdims=True), mask)
            coef = jnp.where(sub == e, jnp.sum(jnp.where(eq, gb, 0.0), axis=0, keepdims=True), coef)
        hit = jnp.broadcast_to(jnp.max(mask, axis=0, keepdims=True), (el, t))
        rank = jnp.dot(hit.astype(jnp.bfloat16), upper, preferred_element_type=jnp.float32)
        mask = jnp.where(rank < cap, mask, 0.0)
        within = jnp.dot(mask.astype(jnp.bfloat16), upper, preferred_element_type=jnp.float32)
        pos = jnp.where(mask > 0.0, within + base, -1.0)
        cum = jnp.where(lane == b, base, cum)
        base = base + jnp.sum(mask, axis=1, keepdims=True)
        pos_ref[:, b * t:(b + 1) * t] = pos
        cols = jnp.transpose(jnp.concatenate([coef, jnp.zeros((128 - el, t), jnp.float32)], axis=0))
        for e in range(el):
            slab[e, b * t:(b + 1) * t, :] = jnp.broadcast_to(cols[:, e:e + 1], (t, 128))
    gates_out = pltpu.make_async_copy(slab, gate_ref, gsem)
    gates_out.start()
    cum_ref[...] = jnp.where(lane == 8, base, cum).astype(jnp.int32)

    pxn, pyn, pdg, pme = [d + 1 - 2 * ic for d in (dxn, dyn, ddg, me)]
    for k, d, h, then in ((0, dxn, 0, (6, 8)), (2, dyn, 1, (7, 10)), (4, pme, 0, ()), (5, pme, 1, ()),
                          (1, dxn, 1, (9,)), (3, dyn, 0, (11,)), (8, pxn, 0, ()), (10, pyn, 1, ()),
                          (9, pxn, 1, ()), (11, pyn, 0, ()), (6, ddg, 0, (12,)), (7, ddg, 1, (13,)),
                          (12, pdg, 0, ()), (13, pdg, 1, ())):
        cs[k].wait_recv()
        for f in then:
            cs[f].start()
        out(d, h)
    for k in range(14):
        cs[k].wait_send()
    for c in mcopies:
        c.wait_send()
    for o in outs + [gates_out]:
        o.wait()


def expert_kernel(cum_ref, pos_ref, gate_ref, x_hbm, w1_ref, w3_ref, w2_ref, acc_ref,
                  w13b, w2b, gb, x_ref, sel, xg, hb, ob, order, sems, xsem):
    el, hd, f = w1_ref.shape
    n = x_hbm.shape[0]
    fm = f // 256 * 256
    ft = f - fm

    def listing(e, k):
        @pl.when(cum_ref[e, 8] > 0)
        def _():
            order[k] = e
        return jnp.where(cum_ref[e, 8] > 0, k + 1, k)

    nact = lax.fori_loop(0, el, listing, 0)

    def up(k):
        e, s = order[k], k % 2
        return [pltpu.make_async_copy(w.at[e, :, pl.ds(c, m)], w13b.at[s, :, pl.ds(o, m)], sems.at[s, j])
                for j, (w, c, m, o) in enumerate(((w1_ref, 0, f, 0), (w3_ref, 0, f, f)))]

    def down(k):
        e, s = order[k], k % 2
        return [pltpu.make_async_copy(w2_ref.at[e], w2b.at[s], sems.at[s, 4]),
                pltpu.make_async_copy(gate_ref.at[e], gb.at[s], sems.at[s, 5])]

    def start(copies, k):
        @pl.when(k < nact)
        def _():
            for c in copies(k):
                c.start()

    start(up, 0)
    xcopy = pltpu.make_async_copy(x_hbm, x_ref, xsem)
    xcopy.start()
    start(down, 0)
    acc_ref[...] = jnp.zeros_like(acc_ref)
    xcopy.wait()

    def wide(g):
        return jnp.concatenate([g] * (hd // 128), axis=1)

    def tile(k, e, s, r0, tm, cnt, dense):
        first = r0 == 0
        r0f = r0.astype(jnp.float32)
        lo = jnp.int32(0)
        hi = jnp.int32(0)
        for b in range(8):
            lo += jnp.where(cum_ref[e, b + 1] <= r0, 1, 0)
            hi += jnp.where(cum_ref[e, b] < r0 + tm, 1, 0)
        span = hi - lo
        bounds = ((0, 3), (3, 4), (4, 5), (5, 8))

        def pick(nb):
            win = nb * 128
            toks = pl.ds(pl.multiple_of(jnp.minimum(lo, 8 - nb) * 128, 128), win)
            p = pos_ref[pl.ds(e, 1), toks]
            rows = lax.broadcasted_iota(jnp.int32, (tm, win), 0).astype(jnp.float32) + r0f
            sel[:tm, :win] = jnp.where(rows == p, 1.0, 0.0).astype(jnp.bfloat16)
            xg[:tm] = jnp.dot(sel[:tm, :win], x_ref[toks, :], preferred_element_type=jnp.float32).astype(xg.dtype)

        if tm == 256:
            @pl.when(dense)
            def _():
                xg[:tm] = x_ref[pl.ds(pl.multiple_of(r0, tm), tm), :]

        for under, nb in bounds:
            @pl.when(jnp.logical_not(dense) & (span > under) & (span <= nb))
            def _():
                pick(nb)

        @pl.when(first)
        def _():
            for c in up(k) + down(k):
                c.wait()
            start(up, k + 1)
            start(down, k + 1)

        def act(a1, a3):
            return (jax.nn.silu(a1) * a3).astype(jnp.bfloat16)

        def mm(c, m):
            return jnp.dot(xg[:tm], w13b[s, :, c:c + m], preferred_element_type=jnp.float32)

        for c in range(0, fm, 256):
            hb[:tm, c:c + 256] = act(mm(c, 256), mm(f + c, 256))
        hb[:tm, fm:] = act(mm(fm, ft), mm(f + fm, ft))
        ob[:tm] = jnp.dot(hb[:tm], w2b[s], preferred_element_type=jnp.float32).astype(jnp.bfloat16)

        if tm == 256:
            @pl.when(dense)
            def _():
                toks = pl.ds(pl.multiple_of(r0, tm), tm)
                g = wide(gb[s, toks, :])
                acc_ref[toks, :] += jnp.where(g > 0.0, g * ob[:tm].astype(jnp.float32), 0.0)

        def put(nb):
            for b0 in range(0, nb, 4):
                m = min(4, nb - b0) * 128
                toks = pl.ds(pl.multiple_of((jnp.minimum(lo, 8 - nb) + b0) * 128, 128), m)
                r = lax.dot_general(sel[:tm, b0 * 128:b0 * 128 + m], ob[:tm], (((0,), (0,)), ((), ())),
                                    preferred_element_type=jnp.float32)
                acc_ref[toks, :] += wide(gb[s, toks, :]) * r

        for under, nb in bounds:
            @pl.when(jnp.logical_not(dense) & (span > under) & (span <= nb))
            def _():
                put(nb)

    def expert(k, c):
        e, s = order[k], k % 2
        cnt = cum_ref[e, 8]
        dense = cnt > 768
        rem = jnp.where(dense, 0, cnt % 256)
        big = jnp.where(dense, n // 256, (cnt + 127) // 256)

        def step(i, c):
            tile(k, e, s, i * 256, 256, cnt, dense)
            return c

        lax.fori_loop(0, big, step, 0)

        @pl.when((rem > 0) & (rem <= 128))
        def _():
            tile(k, e, s, big * 256, 128, cnt, jnp.bool_(False))

        return c

    lax.fori_loop(0, nact, expert, 0)


def scatter_kernel(nc, part_ref, x_ref, y_ref, own, prt, rx, ry, r2, lsem, s0, q0, s1, q1, s2, q2):
    dp, ey, ix, ic, part, xn, yn = place()
    hd = x_ref.shape[1]
    half = hd // 2
    w = half // nc
    barrier = pltpu.get_barrier_semaphore()
    for d in (part, xn, yn):
        pl.semaphore_signal(barrier, inc=1, device_id=d, device_id_type=MESH)

    chunks = [(s, i) for i in range(nc) for s in range(2)]

    def cols(s, i):
        return pl.ds(s * half + i * w, w)

    loads, ph0, ph1, ph2 = {}, {}, {}, {}
    for s, i in chunks:
        k = i * 2 + s
        c = cols(s, i)
        loads[s, i] = pltpu.make_async_copy(part_ref.at[:, :, ic, :, c], own.at[:, :, :, c], lsem.at[k])
        ph0[s, i] = pltpu.make_async_remote_copy(
            src_ref=part_ref.at[:, :, 1 - ic, :, c], dst_ref=prt.at[:, :, :, c], send_sem=s0.at[k],
            recv_sem=q0.at[k], device_id=part, device_id_type=MESH)
        if s == 0:
            ph1[s, i] = pltpu.make_async_remote_copy(
                src_ref=own.at[:, 1 - ix, :, c], dst_ref=rx.at[:, :, pl.ds(i * w, w)], send_sem=s1.at[k],
                recv_sem=q1.at[k], device_id=xn, device_id_type=MESH)
            ph2[s, i] = pltpu.make_async_remote_copy(
                src_ref=own.at[1 - ey, ix, :, c], dst_ref=r2.at[:, c], send_sem=s2.at[k],
                recv_sem=q2.at[k], device_id=yn, device_id_type=MESH)
        else:
            ph1[s, i] = pltpu.make_async_remote_copy(
                src_ref=own.at[1 - ey, :, :, c], dst_ref=ry.at[:, :, pl.ds(i * w, w)], send_sem=s1.at[k],
                recv_sem=q1.at[k], device_id=yn, device_id_type=MESH)
            ph2[s, i] = pltpu.make_async_remote_copy(
                src_ref=own.at[ey, 1 - ix, :, c], dst_ref=r2.at[:, c], send_sem=s2.at[k],
                recv_sem=q2.at[k], device_id=xn, device_id_type=MESH)
    for k in chunks:
        loads[k].start()
    pl.semaphore_wait(barrier, 3)
    for k in chunks:
        ph0[k].start()
    for s, i in chunks:
        c = cols(s, i)
        loads[s, i].wait()
        ph0[s, i].wait_recv()
        if s == 0:
            own[:, 1 - ix, :, c] += prt[:, 1 - ix, :, c]
        else:
            own[1 - ey, :, :, c] += prt[1 - ey, :, :, c]
        ph1[s, i].start()
        if s == 0:
            own[:, ix, :, c] += prt[:, ix, :, c]
        else:
            own[ey, :, :, c] += prt[ey, :, :, c]
    for s, i in chunks:
        c = cols(s, i)
        ph1[s, i].wait_recv()
        if s == 0:
            own[1 - ey, ix, :, c] += rx[1 - ey, :, i * w:(i + 1) * w]
        else:
            own[ey, 1 - ix, :, c] += ry[1 - ix, :, i * w:(i + 1) * w]
        ph2[s, i].start()
        if s == 0:
            own[ey, ix, :, c] += rx[ey, :, i * w:(i + 1) * w]
        else:
            own[ey, ix, :, c] += ry[ix, :, i * w:(i + 1) * w]
    for s, i in chunks:
        c = cols(s, i)
        ph2[s, i].wait_recv()
        y_ref[:, c] = (x_ref[:, c].astype(jnp.float32) + (own[ey, ix, :, c] + r2[:, c])).astype(y_ref.dtype)
    for k in chunks:
        ph0[k].wait_send()
        ph1[k].wait_send()
        ph2[k].wait_send()


def solution(mesh):
    nx = mesh.shape["ex"]
    nd = mesh.shape["ey"] * nx
    tok = P(("dp", "ey", "ex"), None)
    wsp = P(("ey", "ex"), None, None)
    f32 = jnp.float32
    dma = pltpu.SemaphoreType.DMA

    def local(x, ids, gates, w1, w3, w2):
        t, hd = x.shape
        top = ids.shape[1]
        el, _, f = w1.shape
        n = nd * t
        cap = min(t, CAPF * t * top // nd)
        xall, pos, gate, cum = pl.pallas_call(
            functools.partial(gather_kernel, cap),
            out_shape=(jax.ShapeDtypeStruct((n, hd), x.dtype), jax.ShapeDtypeStruct((el, n), f32),
                       jax.ShapeDtypeStruct((el, n, 128), f32), jax.ShapeDtypeStruct((el, 128), jnp.int32)),
            in_specs=[VM] * 3, out_specs=(ANY, VM, ANY, VM),
            scratch_shapes=[pltpu.VMEM((n, hd), x.dtype), pltpu.VMEM((nd, 16, t), f32), pltpu.VMEM((el, n, 128), f32),
                            dma((14,)), dma((14,)), dma((16,)), dma, dma((7,)), dma((7,))],
            compiler_params=pltpu.CompilerParams(collective_id=0, has_side_effects=True),
            name="gather")(x, ids.T, gates.T)
        acc = pl.pallas_call(
            expert_kernel,
            out_shape=jax.ShapeDtypeStruct((n, hd), f32),
            in_specs=[SM, VM, ANY, ANY, ANY, ANY, ANY], out_specs=VM,
            scratch_shapes=[pltpu.VMEM((2, hd, 2 * f), w1.dtype), pltpu.VMEM((2, f, hd), w2.dtype),
                            pltpu.VMEM((2, n, 128), f32), pltpu.VMEM((n, hd), x.dtype),
                            pltpu.VMEM((256, n), x.dtype), pltpu.VMEM((256, hd), x.dtype),
                            pltpu.VMEM((256, f), x.dtype), pltpu.VMEM((256, hd), x.dtype),
                            pltpu.SMEM((el + 2,), jnp.int32), dma((2, 6)), dma],
            compiler_params=pltpu.CompilerParams(vmem_limit_bytes=VLIM),
            name="experts")(cum, pos, gate, xall, w1, w3, w2)
        nc = 4
        half = hd // 2
        y = pl.pallas_call(
            functools.partial(scatter_kernel, nc),
            out_shape=jax.ShapeDtypeStruct((t, hd), x.dtype),
            in_specs=[ANY, VM], out_specs=VM,
            scratch_shapes=[pltpu.VMEM((2, 2, t, hd), f32), pltpu.VMEM((2, 2, t, hd), f32),
                            pltpu.VMEM((2, t, half), f32), pltpu.VMEM((2, t, half), f32),
                            pltpu.VMEM((t, hd), f32)] + [dma((2 * nc,))] * 7,
            compiler_params=pltpu.CompilerParams(collective_id=1, has_side_effects=True),
            name="scatter")(acc.reshape(2, 2, 2, t, hd), x)
        return y

    return jax.shard_map(local, mesh=mesh, in_specs=(tok, tok, tok, wsp, wsp, wsp),
                         out_specs=tok, check_vma=False)
```

```python
import functools

import jax
import jax.numpy as jnp
from jax import lax
from jax.experimental import pallas as pl
from jax.experimental.pallas import tpu as pltpu
from jax.sharding import PartitionSpec as P

CAPF = 2
MESH = pl.DeviceIdType.MESH
ANY = pl.BlockSpec(memory_space=pl.ANY)
VM = pl.BlockSpec(memory_space=pltpu.VMEM)
SM = pl.BlockSpec(memory_space=pltpu.SMEM)
VLIM = 67043328


def place():
    dp, ey, ex = lax.axis_index("dp"), lax.axis_index("ey"), lax.axis_index("ex")
    ix, ic = ex // 2, ex % 2
    part = (dp, ey, ix * 2 + (1 - ic))
    xn = (dp, ey, (1 - ix) * 2 + ic)
    yn = (dp, 1 - ey, ex)
    return dp, ey, ix, ic, part, xn, yn


def gather_kernel(cap, x_ref, ids_ref, gates_ref, out_ref, pos_ref, gate_ref, cum_ref,
                  xall_ref, meta, slab, ssem, rsem, osem, gsem, msend, mrecv):
    t, hd = x_ref.shape
    top = ids_ref.shape[0]
    hf = t // 2
    dp, ey, ix, ic, part, xn, yn = place()
    me = ey * 4 + ix * 2 + ic
    dxn = ey * 4 + (1 - ix) * 2 + ic
    dyn = (1 - ey) * 4 + ix * 2 + ic
    ddg = (1 - ey) * 4 + (1 - ix) * 2 + ic

    def dev(d):
        return (dp, d // 4, d % 4)

    meta[me, :top] = ids_ref[...].astype(jnp.float32)
    meta[me, top:8] = jnp.full((8 - top, t), -1.0, jnp.float32)
    meta[me, 8:8 + top] = gates_ref[...]
    meta[me, 8 + top:] = jnp.zeros((8 - top, t), jnp.float32)

    barrier = pltpu.get_barrier_semaphore()
    for j in range(1, 8):
        pl.semaphore_signal(barrier, inc=1, device_id=dev((me + j) % 8), device_id_type=MESH)
    pl.semaphore_wait(barrier, 7)

    mcopies = []
    for j in range(1, 8):
        c = pltpu.make_async_remote_copy(
            src_ref=meta.at[me], dst_ref=meta.at[me], send_sem=msend.at[j - 1],
            recv_sem=mrecv.at[j - 1], device_id=dev((me + j) % 8), device_id_type=MESH)
        c.start()
        mcopies.append(c)

    def rows(d, h):
        return pl.ds(pl.multiple_of(d * t + h * hf, hf), hf)

    def rc(k, src, d, h, to):
        return pltpu.make_async_remote_copy(
            src_ref=src, dst_ref=xall_ref.at[rows(d, h)], send_sem=ssem.at[k],
            recv_sem=rsem.at[k], device_id=to, device_id_type=MESH)

    def own(k, h, to):
        return rc(k, x_ref.at[pl.ds(h * hf, hf)], me, h, to)

    def fwd(k, d, h, to):
        return rc(k, xall_ref.at[rows(d, h)], d, h, to)

    cs = {0: own(0, 0, xn), 1: own(1, 1, xn), 2: own(2, 1, yn), 3: own(3, 0, yn),
          4: own(4, 0, part), 5: own(5, 1, part),
          6: fwd(6, dxn, 0, yn), 7: fwd(7, dyn, 1, xn),
          8: fwd(8, dxn, 0, part), 9: fwd(9, dxn, 1, part),
          10: fwd(10, dyn, 1, part), 11: fwd(11, dyn, 0, part),
          12: fwd(12, ddg, 0, part), 13: fwd(13, ddg, 1, part)}
    for k in (0, 2, 1, 3, 4, 5):
        cs[k].start()

    outs = []

    def out(d, h):
        src = x_ref.at[pl.ds(h * hf, hf)] if d is None else xall_ref.at[rows(d, h)]
        o = pltpu.make_async_copy(src, out_ref.at[rows(me if d is None else d, h)], osem.at[len(outs)])
        o.start()
        outs.append(o)

    out(None, 0)
    out(None, 1)

    for c in mcopies:
        c.wait_recv()

    el = pos_ref.shape[0]
    ri = lax.broadcasted_iota(jnp.int32, (128, 128), 0)
    ci = lax.broadcasted_iota(jnp.int32, (128, 128), 1)
    upper = (ri < ci).astype(jnp.bfloat16)
    sub = lax.broadcasted_iota(jnp.int32, (el, t), 0)
    lane = lax.broadcasted_iota(jnp.int32, (el, 128), 1)
    base = jnp.zeros((el, 1), jnp.float32)
    cum = jnp.zeros((el, 128), jnp.float32)
    first = (me * el).astype(jnp.float32)
    for b in range(8):
        m = meta[b]
        idb, gb = m[:8], m[8:]
        mask = jnp.zeros((el, t), jnp.float32)
        coef = jnp.zeros((el, t), jnp.float32)
        for e in range(el):
            eq = idb == first + e
            mask = jnp.where(sub == e, jnp.max(jnp.where(eq, 1.0, 0.0), axis=0, keepdims=True), mask)
            coef = jnp.where(sub == e, jnp.sum(jnp.where(eq, gb, 0.0), axis=0, keepdims=True), coef)
        hit = jnp.broadcast_to(jnp.max(mask, axis=0, keepdims=True), (el, t))
        rank = jnp.dot(hit.astype(jnp.bfloat16), upper, preferred_element_type=jnp.float32)
        mask = jnp.where(rank < cap, mask, 0.0)
        within = jnp.dot(mask.astype(jnp.bfloat16), upper, preferred_element_type=jnp.float32)
        pos = jnp.where(mask > 0.0, within + base, -1.0)
        cum = jnp.where(lane == b, base, cum)
        base = base + jnp.sum(mask, axis=1, keepdims=True)
        pos_ref[:, b * t:(b + 1) * t] = pos
        cols = jnp.transpose(jnp.concatenate([coef, jnp.zeros((128 - el, t), jnp.float32)], axis=0))
        for e in range(el):
            slab[e, b * t:(b + 1) * t, :] = jnp.broadcast_to(cols[:, e:e + 1], (t, 128))
    gates_out = pltpu.make_async_copy(slab, gate_ref, gsem)
    gates_out.start()
    cum_ref[...] = jnp.where(lane == 8, base, cum).astype(jnp.int32)

    pxn, pyn, pdg, pme = [d + 1 - 2 * ic for d in (dxn, dyn, ddg, me)]
    for k, d, h, then in ((0, dxn, 0, (6, 8)), (2, dyn, 1, (7, 10)), (4, pme, 0, ()), (5, pme, 1, ()),
                          (1, dxn, 1, (9,)), (3, dyn, 0, (11,)), (8, pxn, 0, ()), (10, pyn, 1, ()),
                          (9, pxn, 1, ()), (11, pyn, 0, ()), (6, ddg, 0, (12,)), (7, ddg, 1, (13,)),
                          (12, pdg, 0, ()), (13, pdg, 1, ())):
        cs[k].wait_recv()
        for f in then:
            cs[f].start()
        out(d, h)
    for k in range(14):
        cs[k].wait_send()
    for c in mcopies:
        c.wait_send()
    for o in outs + [gates_out]:
        o.wait()


def expert_kernel(cum_ref, pos_ref, gate_ref, x_hbm, w1_ref, w3_ref, w2_ref, out_ref, acc_ref,
                  w13b, w2b, gb, x_ref, sel, xg, hb, ob, order, sems, xsem, osem):
    el, hd, f = w1_ref.shape
    n = x_hbm.shape[0]
    fm = f // 256 * 256
    ft = f - fm
    tb = 256

    def largest(e, best):
        return jnp.where(cum_ref[e, 8] > cum_ref[best, 8], e, best)

    big_one = lax.fori_loop(1, el, largest, 0)

    def listing(e, k):
        take = (cum_ref[e, 8] > 0) & (e != big_one)

        @pl.when(take)
        def _():
            order[k] = e
        return jnp.where(take, k + 1, k)

    rest = lax.fori_loop(0, el, listing, 0)
    order[rest] = big_one
    nact = jnp.where(cum_ref[big_one, 8] > 0, rest + 1, 0)
    early = cum_ref[big_one, 8] > 768

    def flush(r0):
        rows = pl.ds(pl.multiple_of(r0, tb), tb)
        return pltpu.make_async_copy(acc_ref.at[rows], out_ref.at[rows], osem.at[r0 // tb])

    def up(k):
        e, s = order[k], k % 2
        return [pltpu.make_async_copy(w.at[e, :, pl.ds(c, m)], w13b.at[s, :, pl.ds(o, m)], sems.at[s, j])
                for j, (w, c, m, o) in enumerate(((w1_ref, 0, f, 0), (w3_ref, 0, f, f)))]

    def down(k):
        e, s = order[k], k % 2
        return [pltpu.make_async_copy(w2_ref.at[e], w2b.at[s], sems.at[s, 4]),
                pltpu.make_async_copy(gate_ref.at[e], gb.at[s], sems.at[s, 5])]

    def start(copies, k):
        @pl.when(k < nact)
        def _():
            for c in copies(k):
                c.start()

    start(up, 0)
    xcopy = pltpu.make_async_copy(x_hbm, x_ref, xsem)
    xcopy.start()
    start(down, 0)
    acc_ref[...] = jnp.zeros_like(acc_ref)
    xcopy.wait()

    def wide(g):
        return jnp.concatenate([g] * (hd // 128), axis=1)

    def tile(k, e, s, r0, tm, cnt, dense):
        first = r0 == 0
        r0f = r0.astype(jnp.float32)
        lo = jnp.int32(0)
        hi = jnp.int32(0)
        for b in range(8):
            lo += jnp.where(cum_ref[e, b + 1] <= r0, 1, 0)
            hi += jnp.where(cum_ref[e, b] < r0 + tm, 1, 0)
        span = hi - lo
        bounds = ((0, 3), (3, 4), (4, 5), (5, 8))

        def pick(nb):
            win = nb * 128
            toks = pl.ds(pl.multiple_of(jnp.minimum(lo, 8 - nb) * 128, 128), win)
            p = pos_ref[pl.ds(e, 1), toks]
            rows = lax.broadcasted_iota(jnp.int32, (tm, win), 0).astype(jnp.float32) + r0f
            sel[:tm, :win] = jnp.where(rows == p, 1.0, 0.0).astype(jnp.bfloat16)
            xg[:tm] = jnp.dot(sel[:tm, :win], x_ref[toks, :], preferred_element_type=jnp.float32).astype(xg.dtype)

        if tm == 256:
            @pl.when(dense)
            def _():
                xg[:tm] = x_ref[pl.ds(pl.multiple_of(r0, tm), tm), :]

        for under, nb in bounds:
            @pl.when(jnp.logical_not(dense) & (span > under) & (span <= nb))
            def _():
                pick(nb)

        @pl.when(first)
        def _():
            for c in up(k):
                c.wait()
            start(up, k + 1)
            for c in down(k):
                c.wait()
            start(down, k + 1)

        def act(a1, a3):
            return (jax.nn.silu(a1) * a3).astype(jnp.bfloat16)

        def mm(c, m):
            return jnp.dot(xg[:tm], w13b[s, :, c:c + m], preferred_element_type=jnp.float32)

        for c in range(0, fm, 256):
            hb[:tm, c:c + 256] = act(mm(c, 256), mm(f + c, 256))
        hb[:tm, fm:] = act(mm(fm, ft), mm(f + fm, ft))
        ob[:tm] = jnp.dot(hb[:tm], w2b[s], preferred_element_type=jnp.float32).astype(jnp.bfloat16)

        if tm == 256:
            @pl.when(dense)
            def _():
                toks = pl.ds(pl.multiple_of(r0, tm), tm)
                g = wide(gb[s, toks, :])
                acc_ref[toks, :] += jnp.where(g > 0.0, g * ob[:tm].astype(jnp.float32), 0.0)

            @pl.when(dense & (k == nact - 1))
            def _():
                flush(r0).start()

        def put(nb):
            for b0 in range(0, nb, 4):
                m = min(4, nb - b0) * 128
                toks = pl.ds(pl.multiple_of((jnp.minimum(lo, 8 - nb) + b0) * 128, 128), m)
                r = lax.dot_general(sel[:tm, b0 * 128:b0 * 128 + m], ob[:tm], (((0,), (0,)), ((), ())),
                                    preferred_element_type=jnp.float32)
                acc_ref[toks, :] += wide(gb[s, toks, :]) * r

        for under, nb in bounds:
            @pl.when(jnp.logical_not(dense) & (span > under) & (span <= nb))
            def _():
                put(nb)

    def expert(k, c):
        e, s = order[k], k % 2
        cnt = cum_ref[e, 8]
        dense = cnt > 768
        rem = jnp.where(dense, 0, cnt % 256)
        big = jnp.where(dense, n // 256, (cnt + 127) // 256)

        def step(i, c):
            tile(k, e, s, i * 256, 256, cnt, dense)
            return c

        lax.fori_loop(0, big, step, 0)

        @pl.when((rem > 0) & (rem <= 128))
        def _():
            tile(k, e, s, big * 256, 128, cnt, jnp.bool_(False))

        return c

    lax.fori_loop(0, nact, expert, 0)

    @pl.when(jnp.logical_not(early))
    def _():
        for i in range(n // tb):
            flush(i * tb).start()

    for i in range(n // tb):
        flush(i * tb).wait()


def scatter_kernel(nc, part_ref, x_ref, y_ref, own, prt, rx, ry, r2, lsem, s0, q0, s1, q1, s2, q2):
    dp, ey, ix, ic, part, xn, yn = place()
    hd = x_ref.shape[1]
    half = hd // 2
    w = half // nc
    barrier = pltpu.get_barrier_semaphore()
    for d in (part, xn, yn):
        pl.semaphore_signal(barrier, inc=1, device_id=d, device_id_type=MESH)

    chunks = [(s, i) for i in range(nc) for s in range(2)]

    def cols(s, i):
        return pl.ds(s * half + i * w, w)

    loads, ph0, ph1, ph2 = {}, {}, {}, {}
    for s, i in chunks:
        k = i * 2 + s
        c = cols(s, i)
        loads[s, i] = pltpu.make_async_copy(part_ref.at[:, :, ic, :, c], own.at[:, :, :, c], lsem.at[k])
        ph0[s, i] = pltpu.make_async_remote_copy(
            src_ref=part_ref.at[:, :, 1 - ic, :, c], dst_ref=prt.at[:, :, :, c], send_sem=s0.at[k],
            recv_sem=q0.at[k], device_id=part, device_id_type=MESH)
        if s == 0:
            ph1[s, i] = pltpu.make_async_remote_copy(
                src_ref=own.at[:, 1 - ix, :, c], dst_ref=rx.at[:, :, pl.ds(i * w, w)], send_sem=s1.at[k],
                recv_sem=q1.at[k], device_id=xn, device_id_type=MESH)
            ph2[s, i] = pltpu.make_async_remote_copy(
                src_ref=own.at[1 - ey, ix, :, c], dst_ref=r2.at[:, c], send_sem=s2.at[k],
                recv_sem=q2.at[k], device_id=yn, device_id_type=MESH)
        else:
            ph1[s, i] = pltpu.make_async_remote_copy(
                src_ref=own.at[1 - ey, :, :, c], dst_ref=ry.at[:, :, pl.ds(i * w, w)], send_sem=s1.at[k],
                recv_sem=q1.at[k], device_id=yn, device_id_type=MESH)
            ph2[s, i] = pltpu.make_async_remote_copy(
                src_ref=own.at[ey, 1 - ix, :, c], dst_ref=r2.at[:, c], send_sem=s2.at[k],
                recv_sem=q2.at[k], device_id=xn, device_id_type=MESH)
    for k in chunks:
        loads[k].start()
    pl.semaphore_wait(barrier, 3)
    for k in chunks:
        ph0[k].start()
    for s, i in chunks:
        c = cols(s, i)
        loads[s, i].wait()
        ph0[s, i].wait_recv()
        if s == 0:
            own[:, 1 - ix, :, c] += prt[:, 1 - ix, :, c]
        else:
            own[1 - ey, :, :, c] += prt[1 - ey, :, :, c]
        ph1[s, i].start()
        if s == 0:
            own[:, ix, :, c] += prt[:, ix, :, c]
        else:
            own[ey, :, :, c] += prt[ey, :, :, c]
    for s, i in chunks:
        c = cols(s, i)
        ph1[s, i].wait_recv()
        if s == 0:
            own[1 - ey, ix, :, c] += rx[1 - ey, :, i * w:(i + 1) * w]
        else:
            own[ey, 1 - ix, :, c] += ry[1 - ix, :, i * w:(i + 1) * w]
        ph2[s, i].start()
        if s == 0:
            own[ey, ix, :, c] += rx[ey, :, i * w:(i + 1) * w]
        else:
            own[ey, ix, :, c] += ry[ix, :, i * w:(i + 1) * w]
    for s, i in chunks:
        c = cols(s, i)
        ph2[s, i].wait_recv()
        y_ref[:, c] = (x_ref[:, c].astype(jnp.float32) + (own[ey, ix, :, c] + r2[:, c])).astype(y_ref.dtype)
    for k in chunks:
        ph0[k].wait_send()
        ph1[k].wait_send()
        ph2[k].wait_send()


def solution(mesh):
    nx = mesh.shape["ex"]
    nd = mesh.shape["ey"] * nx
    tok = P(("dp", "ey", "ex"), None)
    wsp = P(("ey", "ex"), None, None)
    f32 = jnp.float32
    dma = pltpu.SemaphoreType.DMA

    def local(x, ids, gates, w1, w3, w2):
        t, hd = x.shape
        top = ids.shape[1]
        el, _, f = w1.shape
        n = nd * t
        cap = min(t, CAPF * t * top // nd)
        xall, pos, gate, cum = pl.pallas_call(
            functools.partial(gather_kernel, cap),
            out_shape=(jax.ShapeDtypeStruct((n, hd), x.dtype), jax.ShapeDtypeStruct((el, n), f32),
                       jax.ShapeDtypeStruct((el, n, 128), f32), jax.ShapeDtypeStruct((el, 128), jnp.int32)),
            in_specs=[VM] * 3, out_specs=(ANY, VM, ANY, VM),
            scratch_shapes=[pltpu.VMEM((n, hd), x.dtype), pltpu.VMEM((nd, 16, t), f32), pltpu.VMEM((el, n, 128), f32),
                            dma((14,)), dma((14,)), dma((16,)), dma, dma((7,)), dma((7,))],
            compiler_params=pltpu.CompilerParams(collective_id=0, has_side_effects=True),
            name="gather")(x, ids.T, gates.T)
        acc = pl.pallas_call(
            expert_kernel,
            out_shape=jax.ShapeDtypeStruct((n, hd), f32),
            in_specs=[SM, VM, ANY, ANY, ANY, ANY, ANY], out_specs=ANY,
            scratch_shapes=[pltpu.VMEM((n, hd), f32),
                            pltpu.VMEM((2, hd, 2 * f), w1.dtype), pltpu.VMEM((2, f, hd), w2.dtype),
                            pltpu.VMEM((2, n, 128), f32), pltpu.VMEM((n, hd), x.dtype),
                            pltpu.VMEM((256, n), x.dtype), pltpu.VMEM((256, hd), x.dtype),
                            pltpu.VMEM((256, f), x.dtype), pltpu.VMEM((256, hd), x.dtype),
                            pltpu.SMEM((el + 2,), jnp.int32), dma((2, 6)), dma, dma((n // 256,))],
            compiler_params=pltpu.CompilerParams(vmem_limit_bytes=VLIM),
            name="experts")(cum, pos, gate, xall, w1, w3, w2)
        nc = 8
        half = hd // 2
        y = pl.pallas_call(
            functools.partial(scatter_kernel, nc),
            out_shape=jax.ShapeDtypeStruct((t, hd), x.dtype),
            in_specs=[ANY, VM], out_specs=VM,
            scratch_shapes=[pltpu.VMEM((2, 2, t, hd), f32), pltpu.VMEM((2, 2, t, hd), f32),
                            pltpu.VMEM((2, t, half), f32), pltpu.VMEM((2, t, half), f32),
                            pltpu.VMEM((t, hd), f32)] + [dma((2 * nc,))] * 7,
            compiler_params=pltpu.CompilerParams(collective_id=1, has_side_effects=True),
            name="scatter")(acc.reshape(2, 2, 2, t, hd), x)
        return y

    return jax.shard_map(local, mesh=mesh, in_specs=(tok, tok, tok, wsp, wsp, wsp),
                         out_specs=tok, check_vma=False)
```

```python
import functools

import jax
import jax.numpy as jnp
from jax import lax
from jax.experimental import pallas as pl
from jax.experimental.pallas import tpu as pltpu
from jax.sharding import PartitionSpec as P

CAPF = 2
MESH = pl.DeviceIdType.MESH
ANY = pl.BlockSpec(memory_space=pl.ANY)
VM = pl.BlockSpec(memory_space=pltpu.VMEM)
SM = pl.BlockSpec(memory_space=pltpu.SMEM)
VLIM = 67043328


def place():
    dp, ey, ex = lax.axis_index("dp"), lax.axis_index("ey"), lax.axis_index("ex")
    ix, ic = ex // 2, ex % 2
    part = (dp, ey, ix * 2 + (1 - ic))
    xn = (dp, ey, (1 - ix) * 2 + ic)
    yn = (dp, 1 - ey, ex)
    return dp, ey, ix, ic, part, xn, yn


def gather_kernel(cap, x_ref, ids_ref, gates_ref, out_ref, pos_ref, gate_ref, cum_ref,
                  xall_ref, meta, slab, ssem, rsem, osem, gsem, msend, mrecv):
    t, hd = x_ref.shape
    top = ids_ref.shape[0]
    hf = t // 2
    dp, ey, ix, ic, part, xn, yn = place()
    me = ey * 4 + ix * 2 + ic
    dxn = ey * 4 + (1 - ix) * 2 + ic
    dyn = (1 - ey) * 4 + ix * 2 + ic
    ddg = (1 - ey) * 4 + (1 - ix) * 2 + ic

    def dev(d):
        return (dp, d // 4, d % 4)

    meta[me, :top] = ids_ref[...].astype(jnp.float32)
    meta[me, top:8] = jnp.full((8 - top, t), -1.0, jnp.float32)
    meta[me, 8:8 + top] = gates_ref[...]
    meta[me, 8 + top:] = jnp.zeros((8 - top, t), jnp.float32)

    barrier = pltpu.get_barrier_semaphore()
    for j in range(1, 8):
        pl.semaphore_signal(barrier, inc=1, device_id=dev((me + j) % 8), device_id_type=MESH)
    pl.semaphore_wait(barrier, 7)

    mcopies = []
    for j in range(1, 8):
        c = pltpu.make_async_remote_copy(
            src_ref=meta.at[me], dst_ref=meta.at[me], send_sem=msend.at[j - 1],
            recv_sem=mrecv.at[j - 1], device_id=dev((me + j) % 8), device_id_type=MESH)
        c.start()
        mcopies.append(c)

    def rows(d, h):
        return pl.ds(pl.multiple_of(d * t + h * hf, hf), hf)

    def rc(k, src, d, h, to):
        return pltpu.make_async_remote_copy(
            src_ref=src, dst_ref=xall_ref.at[rows(d, h)], send_sem=ssem.at[k],
            recv_sem=rsem.at[k], device_id=to, device_id_type=MESH)

    def own(k, h, to):
        return rc(k, x_ref.at[pl.ds(h * hf, hf)], me, h, to)

    def fwd(k, d, h, to):
        return rc(k, xall_ref.at[rows(d, h)], d, h, to)

    cs = {0: own(0, 0, xn), 1: own(1, 1, xn), 2: own(2, 1, yn), 3: own(3, 0, yn),
          4: own(4, 0, part), 5: own(5, 1, part),
          6: fwd(6, dxn, 0, yn), 7: fwd(7, dyn, 1, xn),
          8: fwd(8, dxn, 0, part), 9: fwd(9, dxn, 1, part),
          10: fwd(10, dyn, 1, part), 11: fwd(11, dyn, 0, part),
          12: fwd(12, ddg, 0, part), 13: fwd(13, ddg, 1, part)}
    for k in (0, 2, 1, 3, 4, 5):
        cs[k].start()

    outs = []

    def out(d, h):
        src = x_ref.at[pl.ds(h * hf, hf)] if d is None else xall_ref.at[rows(d, h)]
        o = pltpu.make_async_copy(src, out_ref.at[rows(me if d is None else d, h)], osem.at[len(outs)])
        o.start()
        outs.append(o)

    out(None, 0)
    out(None, 1)

    for c in mcopies:
        c.wait_recv()

    el = pos_ref.shape[0]
    ri = lax.broadcasted_iota(jnp.int32, (128, 128), 0)
    ci = lax.broadcasted_iota(jnp.int32, (128, 128), 1)
    upper = (ri < ci).astype(jnp.bfloat16)
    sub = lax.broadcasted_iota(jnp.int32, (el, t), 0)
    lane = lax.broadcasted_iota(jnp.int32, (el, 128), 1)
    base = jnp.zeros((el, 1), jnp.float32)
    cum = jnp.zeros((el, 128), jnp.float32)
    first = (me * el).astype(jnp.float32)
    for b in range(8):
        m = meta[b]
        idb, gb = m[:8], m[8:]
        mask = jnp.zeros((el, t), jnp.float32)
        coef = jnp.zeros((el, t), jnp.float32)
        for e in range(el):
            eq = idb == first + e
            mask = jnp.where(sub == e, jnp.max(jnp.where(eq, 1.0, 0.0), axis=0, keepdims=True), mask)
            coef = jnp.where(sub == e, jnp.sum(jnp.where(eq, gb, 0.0), axis=0, keepdims=True), coef)
        hit = jnp.broadcast_to(jnp.max(mask, axis=0, keepdims=True), (el, t))
        rank = jnp.dot(hit.astype(jnp.bfloat16), upper, preferred_element_type=jnp.float32)
        mask = jnp.where(rank < cap, mask, 0.0)
        within = jnp.dot(mask.astype(jnp.bfloat16), upper, preferred_element_type=jnp.float32)
        pos = jnp.where(mask > 0.0, within + base, -1.0)
        cum = jnp.where(lane == b, base, cum)
        base = base + jnp.sum(mask, axis=1, keepdims=True)
        pos_ref[:, b * t:(b + 1) * t] = pos
        cols = jnp.transpose(jnp.concatenate([coef, jnp.zeros((128 - el, t), jnp.float32)], axis=0))
        for e in range(el):
            slab[e, b * t:(b + 1) * t, :] = jnp.broadcast_to(cols[:, e:e + 1], (t, 128))
    gates_out = pltpu.make_async_copy(slab, gate_ref, gsem)
    gates_out.start()
    cum_ref[...] = jnp.where(lane == 8, base, cum).astype(jnp.int32)

    pxn, pyn, pdg, pme = [d + 1 - 2 * ic for d in (dxn, dyn, ddg, me)]
    for k, d, h, then in ((0, dxn, 0, (6, 8)), (2, dyn, 1, (7, 10)), (4, pme, 0, ()), (5, pme, 1, ()),
                          (1, dxn, 1, (9,)), (3, dyn, 0, (11,)), (8, pxn, 0, ()), (10, pyn, 1, ()),
                          (9, pxn, 1, ()), (11, pyn, 0, ()), (6, ddg, 0, (12,)), (7, ddg, 1, (13,)),
                          (12, pdg, 0, ()), (13, pdg, 1, ())):
        cs[k].wait_recv()
        for f in then:
            cs[f].start()
        out(d, h)
    for k in range(14):
        cs[k].wait_send()
    for c in mcopies:
        c.wait_send()
    for o in outs + [gates_out]:
        o.wait()


def expert_kernel(cum_ref, pos_ref, gate_ref, x_hbm, w1_ref, w3_ref, w2_ref, out_ref, acc_ref,
                  w13b, w2b, gb, x_ref, sel, xg, hb, ob, order, sems, psem, xsem, osem):
    el, hd, f = w1_ref.shape
    n = x_hbm.shape[0]
    tb = 256

    def largest(e, best):
        return jnp.where(cum_ref[e, 8] > cum_ref[best, 8], e, best)

    big_one = lax.fori_loop(1, el, largest, 0)

    def runner_up(e, best):
        c = cum_ref[e, 8]
        take = (e != big_one) & (c > best[1])
        return jnp.where(take, e, best[0]), jnp.where(take, c, best[1])

    second, c2 = lax.fori_loop(0, el, runner_up, (jnp.int32(-1), jnp.int32(0)))

    @pl.when(c2 > 0)
    def _():
        order[0] = second

    def listing(e, k):
        take = (cum_ref[e, 8] > 0) & (e != big_one) & (e != second)

        @pl.when(take)
        def _():
            order[k] = e
        return jnp.where(take, k + 1, k)

    rest = lax.fori_loop(0, el, listing, jnp.where(c2 > 0, 1, 0))
    order[rest] = big_one
    nact = jnp.where(cum_ref[big_one, 8] > 0, rest + 1, 0)
    early = cum_ref[big_one, 8] > 768

    def flush(r0):
        rows = pl.ds(pl.multiple_of(r0, tb), tb)
        return pltpu.make_async_copy(acc_ref.at[rows], out_ref.at[rows], osem.at[r0 // tb])

    def up(k):
        e, s = order[k], k % 2
        return [pltpu.make_async_copy(w.at[e, :, pl.ds(c, m)], w13b.at[s, :, pl.ds(o, m)], sems.at[s, j])
                for j, (w, c, m, o) in enumerate(((w1_ref, 0, f, 0), (w3_ref, 0, f, f)))]

    def down(k):
        e, s = order[k], k % 2
        return [pltpu.make_async_copy(w2_ref.at[e], w2b.at[s], sems.at[s, 4]),
                pltpu.make_async_copy(gate_ref.at[e], gb.at[s], sems.at[s, 5])]

    def start(copies, k):
        @pl.when(k < nact)
        def _():
            for c in copies(k):
                c.start()

    cuts = [(c, min(256, f - c)) for c in range(0, f, 256)]

    def piece(i):
        c, m = cuts[i]
        return [pltpu.make_async_copy(w.at[order[0], :, pl.ds(c, m)], w13b.at[0, :, pl.ds(o + c, m)], psem.at[i, q])
                for q, (w, o) in enumerate(((w1_ref, 0), (w3_ref, f)))]

    xcopy = pltpu.make_async_copy(x_hbm, x_ref, xsem)
    xcopy.start()

    @pl.when(nact > 0)
    def _():
        for i in range(3):
            for c in piece(i):
                c.start()

    acc_ref[...] = jnp.zeros_like(acc_ref)
    xcopy.wait()

    def wide(g):
        return jnp.concatenate([g] * (hd // 128), axis=1)

    def tile(k, e, s, r0, tm, cnt, dense, opening=False):
        first = r0 == 0
        r0f = r0.astype(jnp.float32)
        lo = jnp.int32(0)
        hi = jnp.int32(0)
        for b in range(8):
            lo += jnp.where(cum_ref[e, b + 1] <= r0, 1, 0)
            hi += jnp.where(cum_ref[e, b] < r0 + tm, 1, 0)
        span = hi - lo
        bounds = ((0, 3), (3, 4), (4, 5), (5, 8))

        def pick(nb):
            win = nb * 128
            toks = pl.ds(pl.multiple_of(jnp.minimum(lo, 8 - nb) * 128, 128), win)
            p = pos_ref[pl.ds(e, 1), toks]
            rows = lax.broadcasted_iota(jnp.int32, (tm, win), 0).astype(jnp.float32) + r0f
            sel[:tm, :win] = jnp.where(rows == p, 1.0, 0.0).astype(jnp.bfloat16)
            xg[:tm] = jnp.dot(sel[:tm, :win], x_ref[toks, :], preferred_element_type=jnp.float32).astype(xg.dtype)

        if tm == 256:
            @pl.when(dense)
            def _():
                xg[:tm] = x_ref[pl.ds(pl.multiple_of(r0, tm), tm), :]

        for under, nb in bounds:
            @pl.when(jnp.logical_not(dense) & (span > under) & (span <= nb))
            def _():
                pick(nb)

        if not opening:
            @pl.when(first)
            def _():
                for c in up(k):
                    c.wait()
                start(up, k + 1)
                for c in down(k):
                    c.wait()
                start(down, k + 1)

        def act(a1, a3):
            return (jax.nn.silu(a1) * a3).astype(jnp.bfloat16)

        def mm(c, m):
            return jnp.dot(xg[:tm], w13b[s, :, c:c + m], preferred_element_type=jnp.float32)

        for i, (c, m) in enumerate(cuts):
            if opening:
                for cp in piece(i):
                    cp.wait()
                later = piece(i + 3) if i + 3 < len(cuts) else down(k) if i + 3 == len(cuts) else []
                for cp in later:
                    cp.start()
            hb[:tm, c:c + m] = act(mm(c, m), mm(f + c, m))
        if opening:
            for cp in down(k):
                cp.wait()
            start(up, k + 1)
            start(down, k + 1)
        ob[:tm] = jnp.dot(hb[:tm], w2b[s], preferred_element_type=jnp.float32).astype(jnp.bfloat16)

        if tm == 256:
            @pl.when(dense)
            def _():
                toks = pl.ds(pl.multiple_of(r0, tm), tm)
                g = wide(gb[s, toks, :])
                acc_ref[toks, :] += jnp.where(g > 0.0, g * ob[:tm].astype(jnp.float32), 0.0)

            @pl.when(dense & (k == nact - 1))
            def _():
                flush(r0).start()

        def put(nb):
            for b0 in range(0, nb, 4):
                m = min(4, nb - b0) * 128
                toks = pl.ds(pl.multiple_of((jnp.minimum(lo, 8 - nb) + b0) * 128, 128), m)
                r = lax.dot_general(sel[:tm, b0 * 128:b0 * 128 + m], ob[:tm], (((0,), (0,)), ((), ())),
                                    preferred_element_type=jnp.float32)
                acc_ref[toks, :] += wide(gb[s, toks, :]) * r

        for under, nb in bounds:
            @pl.when(jnp.logical_not(dense) & (span > under) & (span <= nb))
            def _():
                put(nb)

    def expert(k, c):
        e, s = order[k], k % 2
        cnt = cum_ref[e, 8]
        dense = cnt > 768
        rem = jnp.where(dense, 0, cnt % 256)
        big = jnp.where(dense, n // 256, (cnt + 127) // 256)

        def step(i, c):
            tile(k, e, s, i * 256, 256, cnt, dense)
            return c

        lax.fori_loop(jnp.where(k == 0, 1, 0), big, step, 0)

        @pl.when((rem > 0) & (rem <= 128) & ((k > 0) | (big > 0)))
        def _():
            tile(k, e, s, big * 256, 128, cnt, jnp.bool_(False))

        return c

    @pl.when(nact > 0)
    def _():
        cnt = cum_ref[order[0], 8]
        tile(jnp.int32(0), order[0], 0, jnp.int32(0), 256, cnt, cnt > 768, opening=True)

    lax.fori_loop(0, nact, expert, 0)

    @pl.when(jnp.logical_not(early))
    def _():
        for i in range(n // tb):
            flush(i * tb).start()

    for i in range(n // tb):
        flush(i * tb).wait()


def scatter_kernel(nc, part_ref, x_ref, y_ref, own, prt, rx, ry, r2, lsem, s0, q0, s1, q1, s2, q2):
    dp, ey, ix, ic, part, xn, yn = place()
    hd = x_ref.shape[1]
    half = hd // 2
    w = half // nc
    barrier = pltpu.get_barrier_semaphore()
    for d in (part, xn, yn):
        pl.semaphore_signal(barrier, inc=1, device_id=d, device_id_type=MESH)

    chunks = [(s, i) for i in range(nc) for s in range(2)]

    def cols(s, i):
        return pl.ds(s * half + i * w, w)

    loads, ph0, ph1, ph2 = {}, {}, {}, {}
    for s, i in chunks:
        k = i * 2 + s
        c = cols(s, i)
        loads[s, i] = pltpu.make_async_copy(part_ref.at[:, :, ic, :, c], own.at[:, :, :, c], lsem.at[k])
        ph0[s, i] = pltpu.make_async_remote_copy(
            src_ref=part_ref.at[:, :, 1 - ic, :, c], dst_ref=prt.at[:, :, :, c], send_sem=s0.at[k],
            recv_sem=q0.at[k], device_id=part, device_id_type=MESH)
        if s == 0:
            ph1[s, i] = pltpu.make_async_remote_copy(
                src_ref=own.at[:, 1 - ix, :, c], dst_ref=rx.at[:, :, pl.ds(i * w, w)], send_sem=s1.at[k],
                recv_sem=q1.at[k], device_id=xn, device_id_type=MESH)
            ph2[s, i] = pltpu.make_async_remote_copy(
                src_ref=own.at[1 - ey, ix, :, c], dst_ref=r2.at[:, c], send_sem=s2.at[k],
                recv_sem=q2.at[k], device_id=yn, device_id_type=MESH)
        else:
            ph1[s, i] = pltpu.make_async_remote_copy(
                src_ref=own.at[1 - ey, :, :, c], dst_ref=ry.at[:, :, pl.ds(i * w, w)], send_sem=s1.at[k],
                recv_sem=q1.at[k], device_id=yn, device_id_type=MESH)
            ph2[s, i] = pltpu.make_async_remote_copy(
                src_ref=own.at[ey, 1 - ix, :, c], dst_ref=r2.at[:, c], send_sem=s2.at[k],
                recv_sem=q2.at[k], device_id=xn, device_id_type=MESH)
    for k in chunks:
        loads[k].start()
    pl.semaphore_wait(barrier, 3)
    for k in chunks:
        ph0[k].start()
    for s, i in chunks:
        c = cols(s, i)
        loads[s, i].wait()
        ph0[s, i].wait_recv()
        if s == 0:
            own[:, 1 - ix, :, c] += prt[:, 1 - ix, :, c]
        else:
            own[1 - ey, :, :, c] += prt[1 - ey, :, :, c]
        ph1[s, i].start()
        if s == 0:
            own[:, ix, :, c] += prt[:, ix, :, c]
        else:
            own[ey, :, :, c] += prt[ey, :, :, c]
    for s, i in chunks:
        c = cols(s, i)
        ph1[s, i].wait_recv()
        if s == 0:
            own[1 - ey, ix, :, c] += rx[1 - ey, :, i * w:(i + 1) * w]
        else:
            own[ey, 1 - ix, :, c] += ry[1 - ix, :, i * w:(i + 1) * w]
        ph2[s, i].start()
        if s == 0:
            own[ey, ix, :, c] += rx[ey, :, i * w:(i + 1) * w]
        else:
            own[ey, ix, :, c] += ry[ix, :, i * w:(i + 1) * w]
    for s, i in chunks:
        c = cols(s, i)
        ph2[s, i].wait_recv()
        y_ref[:, c] = (x_ref[:, c].astype(jnp.float32) + (own[ey, ix, :, c] + r2[:, c])).astype(y_ref.dtype)
    for k in chunks:
        ph0[k].wait_send()
        ph1[k].wait_send()
        ph2[k].wait_send()


def solution(mesh):
    nx = mesh.shape["ex"]
    nd = mesh.shape["ey"] * nx
    tok = P(("dp", "ey", "ex"), None)
    wsp = P(("ey", "ex"), None, None)
    f32 = jnp.float32
    dma = pltpu.SemaphoreType.DMA

    def local(x, ids, gates, w1, w3, w2):
        t, hd = x.shape
        top = ids.shape[1]
        el, _, f = w1.shape
        n = nd * t
        cap = min(t, CAPF * t * top // nd)
        xall, pos, gate, cum = pl.pallas_call(
            functools.partial(gather_kernel, cap),
            out_shape=(jax.ShapeDtypeStruct((n, hd), x.dtype), jax.ShapeDtypeStruct((el, n), f32),
                       jax.ShapeDtypeStruct((el, n, 128), f32), jax.ShapeDtypeStruct((el, 128), jnp.int32)),
            in_specs=[VM] * 3, out_specs=(ANY, VM, ANY, VM),
            scratch_shapes=[pltpu.VMEM((n, hd), x.dtype), pltpu.VMEM((nd, 16, t), f32), pltpu.VMEM((el, n, 128), f32),
                            dma((14,)), dma((14,)), dma((16,)), dma, dma((7,)), dma((7,))],
            compiler_params=pltpu.CompilerParams(collective_id=0, has_side_effects=True),
            name="gather")(x, ids.T, gates.T)
        acc = pl.pallas_call(
            expert_kernel,
            out_shape=jax.ShapeDtypeStruct((n, hd), f32),
            in_specs=[SM, VM, ANY, ANY, ANY, ANY, ANY], out_specs=ANY,
            scratch_shapes=[pltpu.VMEM((n, hd), f32),
                            pltpu.VMEM((2, hd, 2 * f), w1.dtype), pltpu.VMEM((2, f, hd), w2.dtype),
                            pltpu.VMEM((2, n, 128), f32), pltpu.VMEM((n, hd), x.dtype),
                            pltpu.VMEM((256, n), x.dtype), pltpu.VMEM((256, hd), x.dtype),
                            pltpu.VMEM((256, f), x.dtype), pltpu.VMEM((256, hd), x.dtype),
                            pltpu.SMEM((el + 2,), jnp.int32), dma((2, 6)), dma((8, 2)), dma, dma((n // 256,))],
            compiler_params=pltpu.CompilerParams(vmem_limit_bytes=VLIM),
            name="experts")(cum, pos, gate, xall, w1, w3, w2)
        nc = 8
        half = hd // 2
        y = pl.pallas_call(
            functools.partial(scatter_kernel, nc),
            out_shape=jax.ShapeDtypeStruct((t, hd), x.dtype),
            in_specs=[ANY, VM], out_specs=VM,
            scratch_shapes=[pltpu.VMEM((2, 2, t, hd), f32), pltpu.VMEM((2, 2, t, hd), f32),
                            pltpu.VMEM((2, t, half), f32), pltpu.VMEM((2, t, half), f32),
                            pltpu.VMEM((t, hd), f32)] + [dma((2 * nc,))] * 7,
            compiler_params=pltpu.CompilerParams(collective_id=1, has_side_effects=True),
            name="scatter")(acc.reshape(2, 2, 2, t, hd), x)
        return y

    return jax.shard_map(local, mesh=mesh, in_specs=(tok, tok, tok, wsp, wsp, wsp),
                         out_specs=tok, check_vma=False)
```

```python
import functools

import jax
import jax.numpy as jnp
from jax import lax
from jax.experimental import pallas as pl
from jax.experimental.pallas import tpu as pltpu
from jax.sharding import PartitionSpec as P

CAPF = 2
MESH = pl.DeviceIdType.MESH
ANY = pl.BlockSpec(memory_space=pl.ANY)
VM = pl.BlockSpec(memory_space=pltpu.VMEM)
SM = pl.BlockSpec(memory_space=pltpu.SMEM)
VLIM = 67043328


def place():
    dp, ey, ex = lax.axis_index("dp"), lax.axis_index("ey"), lax.axis_index("ex")
    ix, ic = ex // 2, ex % 2
    part = (dp, ey, ix * 2 + (1 - ic))
    xn = (dp, ey, (1 - ix) * 2 + ic)
    yn = (dp, 1 - ey, ex)
    return dp, ey, ix, ic, part, xn, yn


def gather_kernel(cap, x_ref, ids_ref, gates_ref, out_ref, pos_ref, gate_ref, cum_ref,
                  xall_ref, meta, slab, ssem, rsem, osem, gsem, msend, mrecv):
    t, hd = x_ref.shape
    top = ids_ref.shape[0]
    hf = t // 2
    dp, ey, ix, ic, part, xn, yn = place()
    me = ey * 4 + ix * 2 + ic
    dxn = ey * 4 + (1 - ix) * 2 + ic
    dyn = (1 - ey) * 4 + ix * 2 + ic
    ddg = (1 - ey) * 4 + (1 - ix) * 2 + ic

    def dev(d):
        return (dp, d // 4, d % 4)

    meta[me, :top] = ids_ref[...].astype(jnp.float32)
    meta[me, top:8] = jnp.full((8 - top, t), -1.0, jnp.float32)
    meta[me, 8:8 + top] = gates_ref[...]
    meta[me, 8 + top:] = jnp.zeros((8 - top, t), jnp.float32)

    barrier = pltpu.get_barrier_semaphore()
    for j in range(1, 8):
        pl.semaphore_signal(barrier, inc=1, device_id=dev((me + j) % 8), device_id_type=MESH)
    pl.semaphore_wait(barrier, 7)

    mcopies = []
    for j in range(1, 8):
        c = pltpu.make_async_remote_copy(
            src_ref=meta.at[me], dst_ref=meta.at[me], send_sem=msend.at[j - 1],
            recv_sem=mrecv.at[j - 1], device_id=dev((me + j) % 8), device_id_type=MESH)
        c.start()
        mcopies.append(c)

    def rows(d, h):
        return pl.ds(pl.multiple_of(d * t + h * hf, hf), hf)

    def rc(k, src, d, h, to):
        return pltpu.make_async_remote_copy(
            src_ref=src, dst_ref=xall_ref.at[rows(d, h)], send_sem=ssem.at[k],
            recv_sem=rsem.at[k], device_id=to, device_id_type=MESH)

    def own(k, h, to):
        return rc(k, x_ref.at[pl.ds(h * hf, hf)], me, h, to)

    def fwd(k, d, h, to):
        return rc(k, xall_ref.at[rows(d, h)], d, h, to)

    cs = {0: own(0, 0, xn), 1: own(1, 1, xn), 2: own(2, 1, yn), 3: own(3, 0, yn),
          4: own(4, 0, part), 5: own(5, 1, part),
          6: fwd(6, dxn, 0, yn), 7: fwd(7, dyn, 1, xn),
          8: fwd(8, dxn, 0, part), 9: fwd(9, dxn, 1, part),
          10: fwd(10, dyn, 1, part), 11: fwd(11, dyn, 0, part),
          12: fwd(12, ddg, 0, part), 13: fwd(13, ddg, 1, part)}
    for k in (0, 2, 1, 3, 4, 5):
        cs[k].start()

    outs = []

    def out(d, h):
        src = x_ref.at[pl.ds(h * hf, hf)] if d is None else xall_ref.at[rows(d, h)]
        o = pltpu.make_async_copy(src, out_ref.at[rows(me if d is None else d, h)], osem.at[len(outs)])
        o.start()
        outs.append(o)

    out(None, 0)
    out(None, 1)

    for c in mcopies:
        c.wait_recv()

    el = pos_ref.shape[0]
    ri = lax.broadcasted_iota(jnp.int32, (128, 128), 0)
    ci = lax.broadcasted_iota(jnp.int32, (128, 128), 1)
    upper = (ri < ci).astype(jnp.bfloat16)
    sub = lax.broadcasted_iota(jnp.int32, (el, t), 0)
    lane = lax.broadcasted_iota(jnp.int32, (el, 128), 1)
    base = jnp.zeros((el, 1), jnp.float32)
    cum = jnp.zeros((el, 128), jnp.float32)
    first = (me * el).astype(jnp.float32)
    for b in range(8):
        m = meta[b]
        idb, gb = m[:8], m[8:]
        mask = jnp.zeros((el, t), jnp.float32)
        coef = jnp.zeros((el, t), jnp.float32)
        for e in range(el):
            eq = idb == first + e
            mask = jnp.where(sub == e, jnp.max(jnp.where(eq, 1.0, 0.0), axis=0, keepdims=True), mask)
            coef = jnp.where(sub == e, jnp.sum(jnp.where(eq, gb, 0.0), axis=0, keepdims=True), coef)
        hit = jnp.broadcast_to(jnp.max(mask, axis=0, keepdims=True), (el, t))
        rank = jnp.dot(hit.astype(jnp.bfloat16), upper, preferred_element_type=jnp.float32)
        mask = jnp.where(rank < cap, mask, 0.0)
        coef = jnp.where(rank < cap, coef, 0.0)
        within = jnp.dot(mask.astype(jnp.bfloat16), upper, preferred_element_type=jnp.float32)
        pos = jnp.where(mask > 0.0, within + base, -1.0)
        cum = jnp.where(lane == b, base, cum)
        base = base + jnp.sum(mask, axis=1, keepdims=True)
        pos_ref[:, b * t:(b + 1) * t] = pos
        cols = jnp.transpose(jnp.concatenate([coef, jnp.zeros((128 - el, t), jnp.float32)], axis=0))
        for e in range(el):
            slab[e, b * t:(b + 1) * t, :] = jnp.broadcast_to(cols[:, e:e + 1], (t, 128))
    gates_out = pltpu.make_async_copy(slab, gate_ref, gsem)
    gates_out.start()
    cum_ref[...] = jnp.where(lane == 8, base, cum).astype(jnp.int32)

    pxn, pyn, pdg, pme = [d + 1 - 2 * ic for d in (dxn, dyn, ddg, me)]
    for k, d, h, then in ((0, dxn, 0, (6, 8)), (2, dyn, 1, (7, 10)), (4, pme, 0, ()), (5, pme, 1, ()),
                          (1, dxn, 1, (9,)), (3, dyn, 0, (11,)), (8, pxn, 0, ()), (10, pyn, 1, ()),
                          (9, pxn, 1, ()), (11, pyn, 0, ()), (6, ddg, 0, (12,)), (7, ddg, 1, (13,)),
                          (12, pdg, 0, ()), (13, pdg, 1, ())):
        cs[k].wait_recv()
        for f in then:
            cs[f].start()
        out(d, h)
    for k in range(14):
        cs[k].wait_send()
    for c in mcopies:
        c.wait_send()
    for o in outs + [gates_out]:
        o.wait()


def expert_kernel(cum_ref, pos_ref, gate_ref, x_hbm, w1_ref, w3_ref, w2_ref, out_ref, acc_ref,
                  w13b, w2b, gb, x_ref, sel, xg, hb, ob, order, sems, psem, xsem, osem):
    el, hd, f = w1_ref.shape
    n = x_hbm.shape[0]
    tb = 256

    def largest(e, best):
        return jnp.where(cum_ref[e, 8] > cum_ref[best, 8], e, best)

    big_one = lax.fori_loop(1, el, largest, 0)

    def runner_up(e, best):
        c = cum_ref[e, 8]
        take = (e != big_one) & (c > best[1])
        return jnp.where(take, e, best[0]), jnp.where(take, c, best[1])

    second, c2 = lax.fori_loop(0, el, runner_up, (jnp.int32(-1), jnp.int32(0)))

    @pl.when(c2 > 0)
    def _():
        order[0] = second

    def listing(e, k):
        take = (cum_ref[e, 8] > 0) & (e != big_one) & (e != second)

        @pl.when(take)
        def _():
            order[k] = e
        return jnp.where(take, k + 1, k)

    rest = lax.fori_loop(0, el, listing, jnp.where(c2 > 0, 1, 0))
    order[rest] = big_one
    nact = jnp.where(cum_ref[big_one, 8] > 0, rest + 1, 0)
    early = cum_ref[big_one, 8] > 768

    def flush(r0):
        rows = pl.ds(pl.multiple_of(r0, tb), tb)
        return pltpu.make_async_copy(acc_ref.at[rows], out_ref.at[rows], osem.at[r0 // tb])

    def up(k):
        e, s = order[k], k % 2
        return [pltpu.make_async_copy(w.at[e, :, pl.ds(c, m)], w13b.at[s, :, pl.ds(o, m)], sems.at[s, j])
                for j, (w, c, m, o) in enumerate(((w1_ref, 0, f, 0), (w3_ref, 0, f, f)))]

    def down(k):
        e, s = order[k], k % 2
        return [pltpu.make_async_copy(w2_ref.at[e], w2b.at[s], sems.at[s, 4]),
                pltpu.make_async_copy(gate_ref.at[e], gb.at[s], sems.at[s, 5])]

    def start(copies, k):
        @pl.when(k < nact)
        def _():
            for c in copies(k):
                c.start()

    cuts = [(c, min(256, f - c)) for c in range(0, f, 256)]

    def piece(i):
        c, m = cuts[i]
        return [pltpu.make_async_copy(w.at[order[0], :, pl.ds(c, m)], w13b.at[0, :, pl.ds(o + c, m)], psem.at[i, q])
                for q, (w, o) in enumerate(((w1_ref, 0), (w3_ref, f)))]

    xcopy = pltpu.make_async_copy(x_hbm, x_ref, xsem)
    xcopy.start()

    @pl.when(nact > 0)
    def _():
        for i in range(3):
            for c in piece(i):
                c.start()

    acc_ref[...] = jnp.zeros_like(acc_ref)
    xcopy.wait()

    def wide(g):
        return jnp.concatenate([g] * (hd // 128), axis=1)

    def tile(k, e, s, r0, tm, cnt, dense, opening=False):
        first = r0 == 0
        r0f = r0.astype(jnp.float32)
        lo = jnp.int32(0)
        hi = jnp.int32(0)
        for b in range(8):
            lo += jnp.where(cum_ref[e, b + 1] <= r0, 1, 0)
            hi += jnp.where(cum_ref[e, b] < r0 + tm, 1, 0)
        span = hi - lo
        bounds = ((0, 3), (3, 4), (4, 5), (5, 8))

        def pick(nb):
            win = nb * 128
            toks = pl.ds(pl.multiple_of(jnp.minimum(lo, 8 - nb) * 128, 128), win)
            p = pos_ref[pl.ds(e, 1), toks]
            rows = lax.broadcasted_iota(jnp.int32, (tm, win), 0).astype(jnp.float32) + r0f
            sel[:tm, :win] = jnp.where(rows == p, 1.0, 0.0).astype(jnp.bfloat16)
            xg[:tm] = jnp.dot(sel[:tm, :win], x_ref[toks, :], preferred_element_type=jnp.float32).astype(xg.dtype)

        if tm == 256:
            @pl.when(dense)
            def _():
                xg[:tm] = x_ref[pl.ds(pl.multiple_of(r0, tm), tm), :]

        for under, nb in bounds:
            @pl.when(jnp.logical_not(dense) & (span > under) & (span <= nb))
            def _():
                pick(nb)

        if not opening:
            @pl.when(first)
            def _():
                for c in up(k):
                    c.wait()
                start(up, k + 1)
                for c in down(k):
                    c.wait()
                start(down, k + 1)

        def act(a1, a3):
            return (jax.nn.silu(a1) * a3).astype(jnp.bfloat16)

        def mm(c, m):
            return jnp.dot(xg[:tm], w13b[s, :, c:c + m], preferred_element_type=jnp.float32)

        for i, (c, m) in enumerate(cuts):
            if opening:
                for cp in piece(i):
                    cp.wait()
                later = piece(i + 3) if i + 3 < len(cuts) else down(k) if i + 3 == len(cuts) else []
                for cp in later:
                    cp.start()
            hb[:tm, c:c + m] = act(mm(c, m), mm(f + c, m))
        if opening:
            for cp in down(k):
                cp.wait()
            start(up, k + 1)
            start(down, k + 1)
        ob[:tm] = jnp.dot(hb[:tm], w2b[s], preferred_element_type=jnp.float32).astype(jnp.bfloat16)

        if tm == 256:
            @pl.when(dense)
            def _():
                toks = pl.ds(pl.multiple_of(r0, tm), tm)
                g = wide(gb[s, toks, :])
                acc_ref[toks, :] += jnp.where(g > 0.0, g * ob[:tm].astype(jnp.float32), 0.0)

            @pl.when(dense & (k == nact - 1))
            def _():
                flush(r0).start()

        def put(nb):
            for b0 in range(0, nb, 4):
                m = min(4, nb - b0) * 128
                toks = pl.ds(pl.multiple_of((jnp.minimum(lo, 8 - nb) + b0) * 128, 128), m)
                r = lax.dot_general(sel[:tm, b0 * 128:b0 * 128 + m], ob[:tm], (((0,), (0,)), ((), ())),
                                    preferred_element_type=jnp.float32)
                acc_ref[toks, :] += wide(gb[s, toks, :]) * r

        for under, nb in bounds:
            @pl.when(jnp.logical_not(dense) & (span > under) & (span <= nb))
            def _():
                put(nb)

    def expert(k, c):
        e, s = order[k], k % 2
        cnt = cum_ref[e, 8]
        dense = cnt > 768
        rem = jnp.where(dense, 0, cnt % 256)
        big = jnp.where(dense, n // 256, (cnt + 127) // 256)

        def step(i, c):
            tile(k, e, s, i * 256, 256, cnt, dense)
            return c

        lax.fori_loop(jnp.where(k == 0, 1, 0), big, step, 0)

        @pl.when((rem > 0) & (rem <= 128) & ((k > 0) | (big > 0)))
        def _():
            tile(k, e, s, big * 256, 128, cnt, jnp.bool_(False))

        return c

    @pl.when(nact > 0)
    def _():
        cnt = cum_ref[order[0], 8]
        tile(jnp.int32(0), order[0], 0, jnp.int32(0), 256, cnt, cnt > 768, opening=True)

    lax.fori_loop(0, nact, expert, 0)

    @pl.when(jnp.logical_not(early))
    def _():
        for i in range(n // tb):
            flush(i * tb).start()

    for i in range(n // tb):
        flush(i * tb).wait()


def scatter_kernel(nc, part_ref, x_ref, y_ref, own, prt, rx, ry, r2, lsem, s0, q0, s1, q1, s2, q2):
    dp, ey, ix, ic, part, xn, yn = place()
    hd = x_ref.shape[1]
    half = hd // 2
    w = half // nc
    barrier = pltpu.get_barrier_semaphore()
    for d in (part, xn, yn):
        pl.semaphore_signal(barrier, inc=1, device_id=d, device_id_type=MESH)

    chunks = [(s, i) for i in range(nc) for s in range(2)]

    def cols(s, i):
        return pl.ds(s * half + i * w, w)

    loads, ph0, ph1, ph2 = {}, {}, {}, {}
    for s, i in chunks:
        k = i * 2 + s
        c = cols(s, i)
        loads[s, i] = pltpu.make_async_copy(part_ref.at[:, :, ic, :, c], own.at[:, :, :, c], lsem.at[k])
        ph0[s, i] = pltpu.make_async_remote_copy(
            src_ref=part_ref.at[:, :, 1 - ic, :, c], dst_ref=prt.at[:, :, :, c], send_sem=s0.at[k],
            recv_sem=q0.at[k], device_id=part, device_id_type=MESH)
        if s == 0:
            ph1[s, i] = pltpu.make_async_remote_copy(
                src_ref=own.at[:, 1 - ix, :, c], dst_ref=rx.at[:, :, pl.ds(i * w, w)], send_sem=s1.at[k],
                recv_sem=q1.at[k], device_id=xn, device_id_type=MESH)
            ph2[s, i] = pltpu.make_async_remote_copy(
                src_ref=own.at[1 - ey, ix, :, c], dst_ref=r2.at[:, c], send_sem=s2.at[k],
                recv_sem=q2.at[k], device_id=yn, device_id_type=MESH)
        else:
            ph1[s, i] = pltpu.make_async_remote_copy(
                src_ref=own.at[1 - ey, :, :, c], dst_ref=ry.at[:, :, pl.ds(i * w, w)], send_sem=s1.at[k],
                recv_sem=q1.at[k], device_id=yn, device_id_type=MESH)
            ph2[s, i] = pltpu.make_async_remote_copy(
                src_ref=own.at[ey, 1 - ix, :, c], dst_ref=r2.at[:, c], send_sem=s2.at[k],
                recv_sem=q2.at[k], device_id=xn, device_id_type=MESH)
    for k in chunks:
        loads[k].start()
    pl.semaphore_wait(barrier, 3)
    for k in chunks:
        ph0[k].start()
    for s, i in chunks:
        c = cols(s, i)
        loads[s, i].wait()
        ph0[s, i].wait_recv()
        if s == 0:
            own[:, 1 - ix, :, c] += prt[:, 1 - ix, :, c]
        else:
            own[1 - ey, :, :, c] += prt[1 - ey, :, :, c]
        ph1[s, i].start()
        if s == 0:
            own[:, ix, :, c] += prt[:, ix, :, c]
        else:
            own[ey, :, :, c] += prt[ey, :, :, c]
    for s, i in chunks:
        c = cols(s, i)
        ph1[s, i].wait_recv()
        if s == 0:
            own[1 - ey, ix, :, c] += rx[1 - ey, :, i * w:(i + 1) * w]
        else:
            own[ey, 1 - ix, :, c] += ry[1 - ix, :, i * w:(i + 1) * w]
        ph2[s, i].start()
        if s == 0:
            own[ey, ix, :, c] += rx[ey, :, i * w:(i + 1) * w]
        else:
            own[ey, ix, :, c] += ry[ix, :, i * w:(i + 1) * w]
    for s, i in chunks:
        c = cols(s, i)
        ph2[s, i].wait_recv()
        y_ref[:, c] = (x_ref[:, c].astype(jnp.float32) + (own[ey, ix, :, c] + r2[:, c])).astype(y_ref.dtype)
    for k in chunks:
        ph0[k].wait_send()
        ph1[k].wait_send()
        ph2[k].wait_send()


def solution(mesh):
    nx = mesh.shape["ex"]
    nd = mesh.shape["ey"] * nx
    tok = P(("dp", "ey", "ex"), None)
    wsp = P(("ey", "ex"), None, None)
    f32 = jnp.float32
    dma = pltpu.SemaphoreType.DMA

    def local(x, ids, gates, w1, w3, w2):
        t, hd = x.shape
        top = ids.shape[1]
        el, _, f = w1.shape
        n = nd * t
        cap = min(t, CAPF * t * top // nd)
        xall, pos, gate, cum = pl.pallas_call(
            functools.partial(gather_kernel, cap),
            out_shape=(jax.ShapeDtypeStruct((n, hd), x.dtype), jax.ShapeDtypeStruct((el, n), f32),
                       jax.ShapeDtypeStruct((el, n, 128), f32), jax.ShapeDtypeStruct((el, 128), jnp.int32)),
            in_specs=[VM] * 3, out_specs=(ANY, VM, ANY, VM),
            scratch_shapes=[pltpu.VMEM((n, hd), x.dtype), pltpu.VMEM((nd, 16, t), f32), pltpu.VMEM((el, n, 128), f32),
                            dma((14,)), dma((14,)), dma((16,)), dma, dma((7,)), dma((7,))],
            compiler_params=pltpu.CompilerParams(collective_id=0, has_side_effects=True),
            name="gather")(x, ids.T, gates.T)
        acc = pl.pallas_call(
            expert_kernel,
            out_shape=jax.ShapeDtypeStruct((n, hd), f32),
            in_specs=[SM, VM, ANY, ANY, ANY, ANY, ANY], out_specs=ANY,
            scratch_shapes=[pltpu.VMEM((n, hd), f32),
                            pltpu.VMEM((2, hd, 2 * f), w1.dtype), pltpu.VMEM((2, f, hd), w2.dtype),
                            pltpu.VMEM((2, n, 128), f32), pltpu.VMEM((n, hd), x.dtype),
                            pltpu.VMEM((256, n), x.dtype), pltpu.VMEM((256, hd), x.dtype),
                            pltpu.VMEM((256, f), x.dtype), pltpu.VMEM((256, hd), x.dtype),
                            pltpu.SMEM((el + 2,), jnp.int32), dma((2, 6)), dma((8, 2)), dma, dma((n // 256,))],
            compiler_params=pltpu.CompilerParams(vmem_limit_bytes=VLIM),
            name="experts")(cum, pos, gate, xall, w1, w3, w2)
        nc = 8
        half = hd // 2
        y = pl.pallas_call(
            functools.partial(scatter_kernel, nc),
            out_shape=jax.ShapeDtypeStruct((t, hd), x.dtype),
            in_specs=[ANY, VM], out_specs=VM,
            scratch_shapes=[pltpu.VMEM((2, 2, t, hd), f32), pltpu.VMEM((2, 2, t, hd), f32),
                            pltpu.VMEM((2, t, half), f32), pltpu.VMEM((2, t, half), f32),
                            pltpu.VMEM((t, hd), f32)] + [dma((2 * nc,))] * 7,
            compiler_params=pltpu.CompilerParams(collective_id=1, has_side_effects=True),
            name="scatter")(acc.reshape(2, 2, 2, t, hd), x)
        return y

    return jax.shard_map(local, mesh=mesh, in_specs=(tok, tok, tok, wsp, wsp, wsp),
                         out_specs=tok, check_vma=False)
```
